256 devices in a mesh: rows: 64 (over x, z, core), cols: 4 (over y).
Axes of the slice: x: 4, y: 4, z: 8, core: 2. Of those that a mesh axis runs over, the one named last changes fastest.
Arguments:
- leading_scene_data: float32 [2, 8192, 8192], P(None, 'rows', 'cols'), may hold values from -12 to 12, as said below
- trailing_scene_data: float32 [2, 8192, 8192], P(None, 'rows', 'cols'), may hold values from -20 to 20, as said below
- shared_usable_flags: int32 [8192, 8192], P('rows', 'cols'), may hold values 0 or 1
- sweep_of_each_line: int32 [8192], P('rows'), may hold values from 0 to 15, never falling along the last dimension, each value on 1 to 1024 neighbouring positions
Outputs:
- deramped: float32 [2, 8192, 8192], P(None, 'rows', 'cols')
- coherence: float32 [8192, 8192], P('rows', 'cols')
The draws below stay inside these ranges and needn't reach their ends.
Inputs may be any that keep to these rules, and one draw needn't show every extreme that they name: `leading_scene_data`: first scene's parts lie in [-12, 12]. `trailing_scene_data`: second scene's parts lie in [-20, 20]; it is the first scene rotated by a smooth phase plus independent noise. `sweep_of_each_line`: burst ids never fall along the rows; each burst holds 1 to 1024 rows, one exactly that many.
All inputs are finite; a program needn't handle non-finite values.
Results may differ from the reference program's by a relative error of at most 0.0003.
Values sent between devices are 32-bit elements.
A program may use at most 64 MiB of HBM per device.

```python
import math
import jax
import jax.numpy as jnp
import numpy as np
from jax import lax

WIN_R = 32
WIN_C = 8
SWEEP_TALLY = 16
SCENE_LINES = 8192
NC = 8192


def scene_primary(key):
    planes = jnp.clip(jax.random.normal(jax.random.fold_in(key, 11), (2, SCENE_LINES, NC), jnp.float32), -6.0, 6.0)
    return planes


def draw_leading_scene_data(key, part):
    return scene_primary(key)


def draw_trailing_scene_data(key, part):
    planes = scene_primary(key)
    speckle = jnp.clip(jax.random.normal(jax.random.fold_in(key, 12), (2, SCENE_LINES, NC), jnp.float32), -6.0, 6.0)
    slopes = jax.random.uniform(jax.random.fold_in(key, 13), (2,), jnp.float32)
    across_slope_term = 2.0 + 2.0 * slopes[0]
    along_slope_term = 1.5 + 1.5 * slopes[1]
    across_coordinate = (jnp.arange(NC, dtype=jnp.float32) + 0.5) / NC
    along_coordinate = (jnp.arange(SCENE_LINES, dtype=jnp.float32) + 0.5) / SCENE_LINES
    planar_angle_fit = across_slope_term * across_coordinate[None, :] + along_slope_term * SWEEP_TALLY * along_coordinate[:, None]
    cos_part = jnp.cos(planar_angle_fit)
    sine_part = jnp.sin(planar_angle_fit)
    real_b = 0.8 * (planes[0] * cos_part + planes[1] * sine_part) + 0.6 * speckle[0]
    imag_b = 0.8 * (planes[1] * cos_part - planes[0] * sine_part) + 0.6 * speckle[1]
    return jnp.stack([real_b, imag_b])


def touch_ends(array, stream_key, smallest, high):
    spot = [jax.random.randint(jax.random.fold_in(stream_key, axis), (), 0, length) for axis, length in enumerate(array.shape)]
    longest = array.shape.index(max(array.shape))
    neighbour = spot[:longest] + [(spot[longest] + 1) % array.shape[longest]] + spot[longest + 1:]
    return array.at[tuple(spot)].set(smallest).at[tuple(neighbour)].set(high)


def profile(count, total, bound, slope):
    weights = [(1 << 20) // math.isqrt(grade ** slope) + 1 for grade in range(2, count + 1)]
    spare, holding = total - bound - (count - 1), [1] * (count - 1)
    while spare > 0:
        candidates = [i for i in range(count - 1) if holding[i] < bound]
        whole, left = sum([weights[i] for i in candidates]), spare
        for i in candidates:
            addition = min(bound - holding[i], max(1, left * weights[i] // whole), spare)
            holding[i] = holding[i] + addition
            spare = spare - addition
    return np.array([bound] + holding)


def ragged(key, count, total, most, skew):
    if count == 2:
        one = jax.random.randint(key, (), max(1, total - most), min(most, total - 1) + 1)
        return jnp.stack([one, total - one])
    tallies = jnp.asarray(profile(count, total, most, skew), jnp.int32)
    couples = (count - 1) // 2
    source_of, taker = tallies[1:1 + 2 * couples:2], tallies[2:2 + 2 * couples:2]
    slack = jnp.minimum(source_of - 1, most - taker)
    passed = jax.random.randint(jax.random.fold_in(key, 1), (couples,), 0, 1 << 20) % (slack + 1)
    tallies = tallies.at[1:1 + 2 * couples:2].set(source_of - passed).at[2:2 + 2 * couples:2].set(taker + passed)
    return tallies[jax.random.permutation(jax.random.fold_in(key, 2), count)]


def setup_inputs(seed: int = 0) -> dict:
    keys = jax.random.split(jax.random.key(seed), 5)
    leading_scene_data = draw_leading_scene_data(jax.random.fold_in(keys[4], 71), 0)
    trailing_scene_data = draw_trailing_scene_data(jax.random.fold_in(keys[4], 71), 0)
    shared_usable_flags = touch_ends((jax.random.randint(keys[2], (SCENE_LINES, NC), 0, 8) < 7).astype(jnp.int32), jax.random.fold_in(keys[2], 1), 0, 1)
    sweep_of_each_line = jnp.searchsorted(jnp.cumsum(ragged(keys[3], SWEEP_TALLY, SCENE_LINES, 2 * SCENE_LINES // SWEEP_TALLY, 1)), jnp.arange(SCENE_LINES), side="right").astype(jnp.int32)
    return {"leading_scene_data": leading_scene_data, "trailing_scene_data": trailing_scene_data, "shared_usable_flags": shared_usable_flags, "sweep_of_each_line": sweep_of_each_line}


largest_value = lax.Precision.HIGHEST

def box_filter(plane):
    zero_value = jnp.zeros((), plane.dtype)
    return lax.reduce_window(plane, zero_value, lax.add, (WIN_R, WIN_C), (1, 1), ((WIN_R // 2, WIN_R // 2 - 1), (WIN_C // 2, WIN_C // 2 - 1)))

def sweep_aggregates(sweep_membership, line_aggregates):
    return jnp.dot(sweep_membership.T, line_aggregates, precision=largest_value)

def solve_ramps(pixel_count, moment_cc, moment_cr, moment_rr, sums):
    ridge_term = 0.001 * pixel_count + 1.0
    diag_col = moment_cc + ridge_term
    diag_row = moment_rr + ridge_term
    determinant = diag_col * diag_row - moment_cr * moment_cr
    base_part = sums[:, 0:2] / (pixel_count + ridge_term)[:, None]
    col_slope = (diag_row[:, None] * sums[:, 2:4] - moment_cr[:, None] * sums[:, 4:6]) / determinant[:, None]
    row_slope = (diag_col[:, None] * sums[:, 4:6] - moment_cr[:, None] * sums[:, 2:4]) / determinant[:, None]
    return jnp.concatenate([base_part, col_slope, row_slope], 1)

def reference(leading_scene_data, trailing_scene_data, shared_usable_flags, sweep_of_each_line):
    weight = shared_usable_flags.astype(jnp.float32)
    real_a = leading_scene_data[0] * weight
    imag_a = leading_scene_data[1] * weight
    real_b = trailing_scene_data[0] * weight
    imag_b = trailing_scene_data[1] * weight
    boxed_real = box_filter(real_a * real_b + imag_a * imag_b)
    boxed_imag = box_filter(imag_a * real_b - real_a * imag_b)
    boxed_pa = box_filter(real_a * real_a + imag_a * imag_a)
    boxed_pb = box_filter(real_b * real_b + imag_b * imag_b)
    normaliser = jnp.sqrt((boxed_pa + 1.0) * (boxed_pb + 1.0))
    coh_real = boxed_real / normaliser
    coh_imag = boxed_imag / normaliser
    coherence = jnp.sqrt(coh_real * coh_real + coh_imag * coh_imag)
    across_coordinate = (jnp.arange(NC, dtype=jnp.float32) + 0.5) * (2.0 / NC) - 1.0
    along_coordinate = (jnp.arange(SCENE_LINES, dtype=jnp.float32) + 0.5) * (2.0 / SCENE_LINES) - 1.0
    sweep_membership = (sweep_of_each_line[:, None] == jnp.arange(SWEEP_TALLY, dtype=jnp.int32)[None, :]).astype(jnp.float32)
    line_usable_tally = lax.optimization_barrier(jnp.sum(weight, 1))
    along_across_moment = lax.optimization_barrier(jnp.sum(weight * across_coordinate[None, :], 1))
    recentered_aggregates = sweep_aggregates(sweep_membership, jnp.stack([line_usable_tally, along_across_moment, along_coordinate * line_usable_tally], 1))
    pixel_count = recentered_aggregates[:, 0]
    floored = jnp.maximum(pixel_count, 1.0)
    middle_across = recentered_aggregates[:, 1] / floored
    middle_along = recentered_aggregates[:, 2] / floored
    along_displacement = along_coordinate - jnp.dot(sweep_membership, middle_along, precision=largest_value)
    across_displacement = across_coordinate[None, :] - jnp.dot(sweep_membership, middle_across, precision=largest_value)[:, None]
    weighted_u = weight * across_displacement
    line_cross_inphase = lax.optimization_barrier(jnp.sum(weight * coh_real, 1))
    line_cross_quadrature = lax.optimization_barrier(jnp.sum(weight * coh_imag, 1))
    along_coordinate_power_two = lax.optimization_barrier(jnp.sum(weighted_u * across_displacement, 1))
    along_first_moment = lax.optimization_barrier(jnp.sum(weighted_u, 1))
    along_weighted_inphase = lax.optimization_barrier(jnp.sum(weighted_u * coh_real, 1))
    along_weighted_quadrature = lax.optimization_barrier(jnp.sum(weighted_u * coh_imag, 1))
    following_picture = sweep_aggregates(sweep_membership, jnp.stack([along_coordinate_power_two, along_displacement * along_first_moment, along_displacement * along_displacement * line_usable_tally, line_cross_inphase, line_cross_quadrature, along_weighted_inphase, along_weighted_quadrature, along_displacement * line_cross_inphase, along_displacement * line_cross_quadrature], 1))
    planar_trends = solve_ramps(pixel_count, following_picture[:, 0], following_picture[:, 1], following_picture[:, 2], following_picture[:, 3:9])
    for_each_line = jnp.dot(sweep_membership, planar_trends, precision=largest_value)
    model_real = for_each_line[:, 0:1] + for_each_line[:, 2:3] * across_displacement + (for_each_line[:, 4] * along_displacement)[:, None]
    model_imag = for_each_line[:, 1:2] + for_each_line[:, 3:4] * across_displacement + (for_each_line[:, 5] * along_displacement)[:, None]
    out_real = coh_real * model_real + coh_imag * model_imag
    out_imag = coh_imag * model_real - coh_real * model_imag
    return (jnp.stack([out_real, out_imag]), coherence)
```

```python
import functools

import jax
import jax.numpy as jnp
from jax import lax
from jax.experimental import pallas as pl
from jax.experimental.pallas import tpu as pltpu
from jax.sharding import PartitionSpec as P

WIN_R = 32
WIN_C = 8
SWEEP_TALLY = 16
HALO = WIN_R // 2
SIDE = WIN_C // 2
LANES = 128
REACH = 8
MESH = pl.DeviceIdType.MESH
F32 = jnp.float32
BF16 = jnp.bfloat16
EXACT = lax.Precision.HIGHEST


def split_pair(x):
    high = x.astype(BF16)
    return high, (x - high.astype(F32)).astype(BF16)


def lane_of(shape):
    return lax.broadcasted_iota(jnp.int32, shape, 1)


def row_of(shape):
    return lax.broadcasted_iota(jnp.int32, shape, 0)


def gamma_kernel(
    count_rows, count_cols,
    lead, trail, flags, sweep,
    gamma, coefs,
    first, second, weight, planes, boxed, up_out, down_out, above, below, left_out, right_out, left_in, right_in,
    side_boxed, side_planes, band, side_band, tri, halo_planes, sums, membership, table, from_cols, table_rows, from_rows,
    load_sem, row_send, row_recv, col_send, col_recv, ysend, yrecv, rsend, rrecv, token,
):
    rows, cols = weight.shape
    blocks = cols // LANES
    my_row = lax.axis_index("rows")
    my_col = lax.axis_index("cols")

    def at(d_row, d_col):
        return {
            "rows": lax.rem(my_row + d_row + count_rows, count_rows),
            "cols": lax.rem(my_col + d_col + count_cols, count_cols),
        }

    def signal(sem, where):
        pl.semaphore_signal(sem, inc=1, device_id=where, device_id_type=MESH)

    barrier = pltpu.get_barrier_semaphore()
    near = [(a, b) for a in (-1, 0, 1) for b in (-1, 0, 1) if (a, b) != (0, 0)] + [(0, 2)]
    for offset in near:
        signal(barrier, at(*offset))

    loads = []

    def load(low, high, left, right):
        started = []
        window = (pl.ds(low, high - low), pl.ds(left, right - left))
        for source, target in ((lead, first), (trail, second)):
            started.append((source.at[(slice(None),) + window], target.at[(slice(None),) + window]))
        started.append((flags.at[window], weight.at[window]))
        copies = []
        for source, target in started:
            copy = pltpu.make_async_copy(source, target, load_sem.at[len(loads)])
            copy.start()
            loads.append(copy)
            copies.append(copy)
        return copies

    def arrive(copies):
        for copy in copies:
            copy.wait()

    inner = rows - HALO
    edge_loads = load(0, HALO, 0, cols) + load(inner, rows, 0, cols)
    side_loads = load(HALO, inner, 0, LANES) + load(HALO, inner, cols - LANES, cols)
    step = (inner - HALO) // 3
    main_loads = [load(HALO + i * step, HALO + (i + 1) * step, LANES, cols - LANES) for i in range(3)]

    box_row = row_of((rows, 2 * rows))
    box_col = lax.rem(lane_of((rows, 2 * rows)), rows) - box_row
    band[...] = jnp.where((box_col >= -HALO) & (box_col < HALO), 1.0, 0.0).astype(BF16)
    tall = rows + 2 * HALO
    side_row = row_of((rows, 2 * tall))
    side_col = lax.rem(lane_of((rows, 2 * tall)), tall) - side_row
    side_line = side_col + side_row
    side_exists = ((side_line >= HALO) | (my_row > 0)) & ((side_line < rows + HALO) | (my_row < count_rows - 1))
    side_band[...] = jnp.where((side_col >= 0) & (side_col < WIN_R) & side_exists, 1.0, 0.0).astype(BF16)
    tri_row = row_of((2 * HALO, 4 * HALO))
    tri_lane = lane_of((2 * HALO, 4 * HALO))
    tri_col = lax.rem(tri_lane, HALO)
    has_above = jnp.where(my_row > 0, 1.0, 0.0)
    has_below = jnp.where(my_row < count_rows - 1, 1.0, 0.0)
    tri_above = jnp.where((tri_row < HALO) & (tri_lane < 2 * HALO) & (tri_col >= tri_row), has_above, 0.0)
    tri_below = jnp.where((tri_row >= HALO) & (tri_lane >= 2 * HALO) & (tri_col < tri_row - HALO), has_below, 0.0)
    tri[...] = (tri_above + tri_below).astype(BF16)
    along = ((my_row * rows + lane_of((LANES, rows))).astype(F32) + 0.5) * (2.0 / (rows * count_rows)) - 1.0
    burst = row_of((LANES, rows))
    power = burst // SWEEP_TALLY
    chosen = jnp.where((burst - power * SWEEP_TALLY == sweep[...]) & (power < 3), 1.0, 0.0)
    membership[1] = chosen * jnp.where(power == 0, 1.0, jnp.where(power == 1, along, along * along))
    membership[0] = jnp.transpose(jnp.where(burst == sweep[...], 1.0, 0.0))

    lane = lane_of((8, LANES))
    lane16 = lane_of((HALO, LANES))

    def products(row, block):
        here = (pl.ds(row, HALO), pl.ds(block * LANES, LANES))
        w = weight[here].astype(F32)
        real_a, imag_a = first[(0,) + here] * w, first[(1,) + here] * w
        real_b, imag_b = second[(0,) + here] * w, second[(1,) + here] * w
        return (
            real_a * real_b + imag_a * imag_b,
            imag_a * real_b - real_a * imag_b,
            real_a * real_a + imag_a * imag_a,
            real_b * real_b + imag_b * imag_b,
        )

    def fill(row, sends=None):
        for block in range(blocks):
            here = pl.ds(block * LANES, LANES)
            for p, x in enumerate(products(row, block)):
                if sends is not None:
                    sends[p, :, here] = x
                high, low = split_pair(x)
                planes[p, pl.ds(row, HALO), here] = high
                planes[p, pl.ds(rows + row, HALO), here] = low

    arrive(edge_loads)
    fill(0, up_out)
    fill(inner, down_out)
    arrive(side_loads)

    @pl.loop(0, rows // HALO)
    def _(group):
        row = pl.multiple_of(group * HALO, HALO)
        packed_left = jnp.zeros((HALO, LANES), F32)
        packed_right = jnp.zeros((HALO, LANES), F32)
        for p, x in enumerate(products(row, 0)):
            x = jnp.where(lane16 < SIDE, x, 0.0)
            packed_left += x if p == 0 else pltpu.roll(x, SIDE * p, 1)
        for p, x in enumerate(products(row, blocks - 1)):
            packed_right += pltpu.roll(jnp.where(lane16 >= LANES - SIDE, x, 0.0), SIDE * (p + 1), 1)
        left_out[pl.ds(row, HALO), :] = packed_left
        right_out[pl.ds(row, HALO), :] = packed_right

    pl.semaphore_wait(barrier, len(near))

    def send(source, target, send_sem, recv_sem, where):
        copy = pltpu.make_async_remote_copy(
            src_ref=source, dst_ref=target, send_sem=send_sem, recv_sem=recv_sem, device_id=where, device_id_type=MESH
        )
        copy.start()
        return copy

    row_copies = [
        send(up_out, below, row_send.at[0], row_recv.at[0], at(-1, 0)),
        send(down_out, above, row_send.at[1], row_recv.at[1], at(1, 0)),
    ]
    col_copies = []
    for source, target, d_col in ((left_out, right_in, -1), (right_out, left_in, 1)):
        for low, size, to, d_row in ((0, rows, HALO, 0), (0, HALO, rows + HALO, -1), (inner, HALO, 0, 1)):
            i = len(col_copies)
            col_copies.append(
                send(
                    source.at[pl.ds(low, size), :], target.at[pl.ds(to, size), :],
                    col_send.at[i], col_recv.at[i], at(d_row, d_col),
                )
            )
    for d in (-1, 1):
        signal(token.at[0], at(d, 0))

    for i, copies in enumerate(main_loads):
        arrive(copies)

        @pl.loop(HALO + i * step, HALO + (i + 1) * step, step=HALO)
        def _(row):
            fill(pl.multiple_of(row, HALO))

    pl.semaphore_wait(token.at[0], 2)
    for d in (-2, 2):
        signal(token.at[1], at(d, 0))

    wide = 2 * LANES
    for p in range(4):
        @pl.loop(0, cols // wide)
        def _(n):
            here = pl.ds(pl.multiple_of(n * wide, wide), wide)
            boxed[p, :, here] = jnp.dot(band[...], planes[p, :, here], preferred_element_type=F32)

    for copy in col_copies:
        copy.wait()
    for i, (arrived, exists) in enumerate(((left_in, my_col > 0), (right_in, my_col < count_cols - 1))):
        high, low = split_pair(arrived[...] * jnp.where(exists, 1.0, 0.0))
        side_planes[pl.ds(0, tall), pl.ds(i * LANES, LANES)] = high
        side_planes[pl.ds(tall, tall), pl.ds(i * LANES, LANES)] = low
    side_boxed[...] = jnp.dot(side_band[...], side_planes[...], preferred_element_type=F32)

    across_first = ((my_col * cols + lane).astype(F32) + 0.5) * (2.0 / (cols * count_cols)) - 1.0

    def finish(group):
        here = pl.ds(pl.multiple_of(group * 8, 8), 8)
        packed = side_boxed[here, pl.ds(0, LANES)], side_boxed[here, pl.ds(LANES, LANES)]

        def block(p, j):
            if j == 0:
                return pltpu.roll(packed[0], LANES - SIDE * (p + 1), 1)
            if j == blocks + 1:
                return packed[1] if p == 0 else pltpu.roll(packed[1], LANES - SIDE * p, 1)
            return boxed[p, here, pl.ds((j - 1) * LANES, LANES)]

        one, one_turned, two, two_turned, four_turned = ({} for _ in range(5))
        raw, raw_turned = {}, {}
        totals = [jnp.zeros((8, LANES), F32) for _ in range(7)]
        for j in range(blocks + 2):
            for p in range(4):
                raw[p, j] = block(p, j)
                raw_turned[p, j] = pltpu.roll(raw[p, j], LANES - 1, 1)
                ready = [j - 1] if j else []
                if j == blocks + 1:
                    ready.append(j)
                for k in ready:
                    follow = raw_turned[p, min(k + 1, j)]
                    one[p, k] = raw[p, k] + jnp.where(lane < LANES - 1, raw_turned[p, k], follow)
                    one_turned[p, k] = pltpu.roll(one[p, k], LANES - 2, 1)
                    if k:
                        i = k - 1
                        two[p, i] = one[p, i] + jnp.where(lane < LANES - 2, one_turned[p, i], one_turned[p, k])
                        two_turned[p, i] = pltpu.roll(two[p, i], SIDE, 1)
            done = [j - 2] if j >= 3 else []
            if j == blocks + 1:
                done.append(j - 1)
            for i in done:
                real, imag, power_a, power_b = (
                    two[p, i] + jnp.where(lane >= SIDE, two_turned[p, i], two_turned[p, i - 1]) for p in range(4)
                )
                scale = lax.rsqrt((power_a + 1.0) * (power_b + 1.0))
                real, imag = real * scale, imag * scale
                there = pl.ds((i - 1) * LANES, LANES)
                gamma[0, here, there] = real
                gamma[1, here, there] = imag
                w = weight[here, there].astype(F32)
                across = across_first + (i - 1) * (LANES * 2.0 / (cols * count_cols))
                wu = w * across
                terms = (w, wu, wu * across, w * real, w * imag, wu * real, wu * imag)
                totals = [total + term for total, term in zip(totals, terms)]
        for q, total in enumerate(totals):
            sums[here, pl.ds(q * LANES, LANES)] = total

    @pl.loop(HALO // 8, inner // 8)
    def _(group):
        finish(group)

    pl.semaphore_wait(token.at[1], 2)
    for d in (-4, 4):
        signal(token.at[2], at(d, 0))

    for copy in row_copies:
        copy.wait()
    for p in range(4):
        for i, arrived in enumerate((above, below)):
            high, low = split_pair(arrived[p])
            halo_planes[p, pl.ds(2 * i * HALO, HALO), :] = high
            halo_planes[p, pl.ds((2 * i + 1) * HALO, HALO), :] = low

        @pl.loop(0, cols // wide)
        def _(n):
            there = pl.ds(pl.multiple_of(n * wide, wide), wide)
            extra = jnp.dot(tri[...], halo_planes[p, :, there], preferred_element_type=F32)
            boxed[p, pl.ds(0, HALO), there] += extra[:HALO]
            boxed[p, pl.ds(inner, HALO), there] += extra[HALO:]

    @pl.loop(0, 2 * HALO // 8)
    def _(i):
        finish(jnp.where(i < HALO // 8, i, i + (inner - HALO) // 8))

    by_burst = jnp.dot(membership[1], sums[...], preferred_element_type=F32, precision=EXACT)
    kind = lane_of((8, 7 * LANES)) // LANES
    pick = jnp.where(kind == row_of((8, 7 * LANES)), 1.0, 0.0)
    table[...] = lax.dot_general(
        pick, by_burst, (((1,), (1,)), ((), ())), preferred_element_type=F32, precision=EXACT
    )

    copies = [
        send(table, from_cols.at[k - 1], ysend.at[k - 1], yrecv.at[k - 1], at(0, k)) for k in range(1, 4)
    ]
    pl.semaphore_wait(token.at[2], 2)
    for copy in copies:
        copy.wait()
    table_rows[...] = (table[...] + from_cols[0]) + (from_cols[1] + from_cols[2])
    distances = [d for k in range(1, REACH + 1) for d in (-k, k)]
    copies = [
        send(table_rows, from_rows.at[i], rsend.at[i], rrecv.at[i], at(d, 0)) for i, d in enumerate(distances)
    ]
    for copy in copies:
        copy.wait()
    total = table_rows[...]
    for i in range(len(distances)):
        total = total + from_rows[i]

    once = pltpu.roll(total, LANES - SWEEP_TALLY, 1)
    twice = pltpu.roll(total, LANES - 2 * SWEEP_TALLY, 1)
    count, sum_u, sum_uu, h0_re, h0_im, hu_re, hu_im = (total[q:q + 1] for q in range(7))
    sum_v, sum_uv, hv_re, hv_im = (once[q:q + 1] for q in (0, 1, 3, 4))
    sum_vv = twice[0:1]
    floored = jnp.maximum(count, 1.0)
    mean_u = sum_u / floored
    mean_v = sum_v / floored
    guu = sum_uu - 2.0 * mean_u * sum_u + mean_u * mean_u * count
    guv = sum_uv - mean_u * sum_v - mean_v * sum_u + mean_u * mean_v * count
    gvv = sum_vv - 2.0 * mean_v * sum_v + mean_v * mean_v * count
    ridge = 0.001 * count + 1.0
    diag_u = guu + ridge
    diag_v = gvv + ridge
    inverse = 1.0 / (diag_u * diag_v - guv * guv)
    base = 1.0 / (count + ridge)
    out = []
    slopes_u, slopes_v = [], []
    for h0, hu, hv in ((h0_re, hu_re, hv_re), (h0_im, hu_im, hv_im)):
        hu = hu - mean_u * h0
        hv = hv - mean_v * h0
        out.append(h0 * base)
        slopes_u.append((diag_v * hu - guv * hv) * inverse)
        slopes_v.append((diag_u * hv - guv * hu) * inverse)
    entries = out + slopes_u + slopes_v + [mean_u, mean_v]
    stacked = jnp.zeros((LANES, LANES), F32)
    place = row_of((LANES, LANES))
    for i, entry in enumerate(entries):
        stacked = jnp.where(place == i, entry, stacked)
    stacked = jnp.where(lane_of((LANES, LANES)) < SWEEP_TALLY, stacked, 0.0)
    coefs[...] = lax.dot_general(
        membership[0], stacked, (((1,), (1,)), ((), ())), preferred_element_type=F32, precision=EXACT
    )


def ramp_kernel(count_rows, count_cols, gamma, coefs, deramped, coherence, out, size, sem):
    _, rows, cols = gamma.shape
    my_row = lax.axis_index("rows")
    my_col = lax.axis_index("cols")
    lane = lane_of((8, LANES))
    across_first = ((my_col * cols + lane).astype(F32) + 0.5) * (2.0 / (cols * count_cols)) - 1.0
    chunk = 32
    copies = []
    for low in range(0, rows, chunk):
        @pl.loop(low // 8, (low + chunk) // 8)
        def _(group):
            start = pl.multiple_of(group * 8, 8)
            here = pl.ds(start, 8)
            line = coefs[here, :]
            along = ((my_row * rows + start + row_of((8, LANES))).astype(F32) + 0.5) * (
                2.0 / (rows * count_rows)
            ) - 1.0
            wide = [jnp.broadcast_to(line[:, q:q + 1], (8, LANES)) for q in range(8)]
            along = along - wide[7]
            base_re = wide[0] + wide[4] * along
            base_im = wide[1] + wide[5] * along
            centred = across_first - wide[6]
            for j in range(cols // LANES):
                there = pl.ds(j * LANES, LANES)
                du = centred + j * (LANES * 2.0 / (cols * count_cols))
                model_re = base_re + wide[2] * du
                model_im = base_im + wide[3] * du
                real, imag = gamma[0, here, there], gamma[1, here, there]
                out[0, here, there] = real * model_re + imag * model_im
                out[1, here, there] = imag * model_re - real * model_im
                size[here, there] = jnp.sqrt(real * real + imag * imag)

        here = pl.ds(low, chunk)
        for source, target in ((out.at[:, here, :], deramped.at[:, here, :]), (size.at[here, :], coherence.at[here, :])):
            copy = pltpu.make_async_copy(source, target, sem.at[len(copies)])
            copy.start()
            copies.append(copy)
    for copy in copies:
        copy.wait()


def on_device(count_rows, count_cols, lead, trail, flags, sweep):
    rows, cols = flags.shape
    tall = rows + 2 * HALO
    vmem = pl.BlockSpec(memory_space=pltpu.VMEM)
    hbm = pl.BlockSpec(memory_space=pl.ANY)
    dma = pltpu.SemaphoreType.DMA
    V = pltpu.VMEM
    gamma, coefs = pl.pallas_call(
        functools.partial(gamma_kernel, count_rows, count_cols),
        out_shape=(V((2, rows, cols), F32), V((rows, LANES), F32)),
        in_specs=[hbm, hbm, hbm, vmem],
        out_specs=(vmem, vmem),
        scratch_shapes=[
            V((2, rows, cols), F32), V((2, rows, cols), F32), V((rows, cols), jnp.int32),
            V((4, 2 * rows, cols), BF16), V((4, rows, cols), F32),
            V((4, HALO, cols), F32), V((4, HALO, cols), F32), V((4, HALO, cols), F32), V((4, HALO, cols), F32),
            V((rows, LANES), F32), V((rows, LANES), F32), V((tall, LANES), F32), V((tall, LANES), F32),
            V((rows, 2 * LANES), F32), V((2 * tall, 2 * LANES), BF16),
            V((rows, 2 * rows), BF16), V((rows, 2 * tall), BF16), V((2 * HALO, 4 * HALO), BF16),
            V((4, 4 * HALO, cols), BF16), V((rows, 7 * LANES), F32), V((2, LANES, rows), F32),
            V((8, LANES), F32), V((3, 8, LANES), F32), V((8, LANES), F32), V((2 * REACH, 8, LANES), F32),
            dma((21,)), dma((2,)), dma((2,)), dma((6,)), dma((6,)), dma((3,)), dma((3,)),
            dma((2 * REACH,)), dma((2 * REACH,)), pltpu.SemaphoreType.REGULAR((3,)),
        ],
        compiler_params=pltpu.CompilerParams(
            collective_id=0, has_side_effects=True, vmem_limit_bytes=40 * 1024 * 1024
        ),
        name="coherence",
    )(lead, trail, flags, sweep.reshape(1, rows))
    return pl.pallas_call(
        functools.partial(ramp_kernel, count_rows, count_cols),
        out_shape=(
            jax.ShapeDtypeStruct((2, rows, cols), F32),
            jax.ShapeDtypeStruct((rows, cols), F32),
        ),
        in_specs=[vmem, vmem],
        out_specs=(hbm, hbm),
        scratch_shapes=[V((2, rows, cols), F32), V((rows, cols), F32), dma((8,))],
        compiler_params=pltpu.CompilerParams(vmem_limit_bytes=16 * 1024 * 1024),
        name="ramp",
    )(gamma, coefs)


def solution(mesh):
    in_specs = (P(None, "rows", "cols"), P(None, "rows", "cols"), P("rows", "cols"), P("rows"))
    out_specs = (P(None, "rows", "cols"), P("rows", "cols"))
    body = functools.partial(on_device, mesh.shape["rows"], mesh.shape["cols"])
    return jax.shard_map(body, mesh=mesh, in_specs=in_specs, out_specs=out_specs, check_vma=False)
```

```python
import functools

import jax
import jax.numpy as jnp
from jax import lax
from jax.experimental import pallas as pl
from jax.experimental.pallas import tpu as pltpu
from jax.sharding import PartitionSpec as P

WIN_R = 32
WIN_C = 8
SWEEP_TALLY = 16
HALO = WIN_R // 2
SIDE = WIN_C // 2
LANES = 128
REACH = 8
MESH = pl.DeviceIdType.MESH
F32 = jnp.float32
BF16 = jnp.bfloat16
EXACT = lax.Precision.HIGHEST


def split_pair(x):
    high = x.astype(BF16)
    return high, (x - high.astype(F32)).astype(BF16)


def lane_of(shape):
    return lax.broadcasted_iota(jnp.int32, shape, 1)


def row_of(shape):
    return lax.broadcasted_iota(jnp.int32, shape, 0)


def gamma_kernel(
    count_rows, count_cols,
    lead, trail, flags, sweep_in,
    gamma, coefs,
    first, second, weight, sweep, planes, up_out, down_out, above, below, left_out, right_out, left_in, right_in,
    side_boxed, side_planes, corner_planes, band, tri, halo_planes, across_box, across_join,
    high_in, low_in, join_in, box_in, own_edge, high_edge, low_edge, join_edge, box_edge,
    sums, membership, table, from_cols, table_rows, from_rows,
    load_sem, row_send, row_recv, col_send, col_recv, ysend, yrecv, rsend, rrecv, token,
):
    rows, cols = weight.shape
    blocks = cols // LANES
    my_row = lax.axis_index("rows")
    my_col = lax.axis_index("cols")

    def at(d_row, d_col):
        return {
            "rows": lax.rem(my_row + d_row + count_rows, count_rows),
            "cols": lax.rem(my_col + d_col + count_cols, count_cols),
        }

    def signal(sem, where):
        pl.semaphore_signal(sem, inc=1, device_id=where, device_id_type=MESH)

    barrier = pltpu.get_barrier_semaphore()
    near = [(a, b) for a in (-1, 0, 1) for b in (-1, 0, 1) if (a, b) != (0, 0)] + [(0, 2)]
    for offset in near:
        signal(barrier, at(*offset))

    loads = []

    def load(low, high, left, right):
        started = []
        window = (pl.ds(low, high - low), pl.ds(left, right - left))
        for source, target in ((lead, first), (trail, second)):
            started.append((source.at[(slice(None),) + window], target.at[(slice(None),) + window]))
        started.append((flags.at[window], weight.at[window]))
        copies = []
        for source, target in started:
            copy = pltpu.make_async_copy(source, target, load_sem.at[len(loads)])
            copy.start()
            loads.append(copy)
            copies.append(copy)
        return copies

    def arrive(copies):
        for copy in copies:
            copy.wait()

    inner = rows - HALO
    edge_loads = load(0, HALO, 0, cols) + load(inner, rows, 0, cols)
    side_loads = load(HALO, inner, 0, LANES) + load(HALO, inner, cols - LANES, cols)
    step = (inner - HALO) // 3
    sweep_load = pltpu.make_async_copy(sweep_in, sweep, load_sem.at[len(loads)])
    sweep_load.start()
    loads.append(sweep_load)
    main_loads = [load(HALO + i * step, HALO + (i + 1) * step, LANES, cols - LANES) for i in range(3)]

    box_row = row_of((rows, 2 * rows))
    box_col = lax.rem(lane_of((rows, 2 * rows)), rows) - box_row
    band[...] = jnp.where((box_col >= -HALO) & (box_col < HALO), 1.0, 0.0).astype(BF16)
    tri_row = row_of((2 * HALO, 4 * HALO))
    tri_lane = lane_of((2 * HALO, 4 * HALO))
    tri_col = lax.rem(tri_lane, HALO)
    has_above = jnp.where(my_row > 0, 1.0, 0.0)
    has_below = jnp.where(my_row < count_rows - 1, 1.0, 0.0)
    tri_above = jnp.where((tri_row < HALO) & (tri_lane < 2 * HALO) & (tri_col >= tri_row), has_above, 0.0)
    tri_below = jnp.where((tri_row >= HALO) & (tri_lane >= 2 * HALO) & (tri_col < tri_row - HALO), has_below, 0.0)
    tri[...] = (tri_above + tri_below).astype(BF16)
    wide = 2 * LANES
    from_lane = row_of((wide, wide))
    to_lane = lane_of((wide, wide))
    apart = from_lane - to_lane
    across_box[...] = jnp.where((apart >= -SIDE) & (apart < SIDE), 1.0, 0.0).astype(BF16)
    from_lane = lax.rem(from_lane, LANES)
    before = (from_lane >= LANES - SIDE) & (to_lane <= from_lane - (LANES - SIDE))
    after = (from_lane < SIDE - 1) & (to_lane >= wide - SIDE + 1 + from_lane)
    across_join[...] = jnp.where(before | after, 1.0, 0.0).astype(BF16)

    lane = lane_of((8, LANES))
    lane16 = lane_of((HALO, LANES))

    def products(row, block):
        here = (pl.ds(row, HALO), pl.ds(block * LANES, LANES))
        w = weight[here].astype(F32)
        real_a, imag_a = first[(0,) + here] * w, first[(1,) + here] * w
        real_b, imag_b = second[(0,) + here] * w, second[(1,) + here] * w
        return (
            real_a * real_b + imag_a * imag_b,
            imag_a * real_b - real_a * imag_b,
            real_a * real_a + imag_a * imag_a,
            real_b * real_b + imag_b * imag_b,
        )

    def fill(row, sends=None):
        for block in range(blocks):
            here = pl.ds(block * LANES, LANES)
            for p, x in enumerate(products(row, block)):
                if sends is not None:
                    sends[p, :, here] = x
                high, low = split_pair(x)
                planes[p, pl.ds(row, HALO), here] = high
                planes[p, pl.ds(rows + row, HALO), here] = low

    def pack(row):
        packed_left = jnp.zeros((HALO, LANES), F32)
        packed_right = jnp.zeros((HALO, LANES), F32)
        for p, x in enumerate(products(row, 0)):
            x = jnp.where(lane16 < SIDE, x, 0.0)
            packed_left += x if p == 0 else pltpu.roll(x, SIDE * p, 1)
        for p, x in enumerate(products(row, blocks - 1)):
            packed_right += pltpu.roll(jnp.where(lane16 >= LANES - SIDE, x, 0.0), SIDE * (p + 1), 1)
        left_out[pl.ds(row, HALO), :] = packed_left
        right_out[pl.ds(row, HALO), :] = packed_right

    arrive(edge_loads)
    pack(0)
    pack(inner)
    fill(0, up_out)
    fill(inner, down_out)
    pl.semaphore_wait(barrier, len(near))

    def send(source, target, send_sem, recv_sem, where):
        copy = pltpu.make_async_remote_copy(
            src_ref=source, dst_ref=target, send_sem=send_sem, recv_sem=recv_sem, device_id=where, device_id_type=MESH
        )
        copy.start()
        return copy

    col_copies, corner_copies = [], []

    def send_side(copies, source, target, low, size, to, d_row, d_col):
        i = len(col_copies) + len(corner_copies)
        copies.append(
            send(
                source.at[pl.ds(low, size), :], target.at[pl.ds(to, size), :],
                col_send.at[i], col_recv.at[i], at(d_row, d_col),
            )
        )

    sides = ((left_out, right_in, -1), (right_out, left_in, 1))
    for source, target, d_col in sides:
        send_side(corner_copies, source, target, 0, HALO, rows + HALO, -1, d_col)
        send_side(corner_copies, source, target, inner, HALO, 0, 1, d_col)
    row_copies = [
        send(up_out, below, row_send.at[0], row_recv.at[0], at(-1, 0)),
        send(down_out, above, row_send.at[1], row_recv.at[1], at(1, 0)),
    ]
    arrive(side_loads)
    for row in range(HALO, inner, HALO):
        pack(row)
    for source, target, d_col in sides:
        send_side(col_copies, source, target, 0, rows, HALO, 0, d_col)
    for d in (-1, 1):
        signal(token.at[0], at(d, 0))

    for i, copies in enumerate(main_loads):
        arrive(copies)

        @pl.loop(HALO + i * step, HALO + (i + 1) * step, step=HALO)
        def _(row):
            fill(pl.multiple_of(row, HALO))

    pl.semaphore_wait(token.at[0], 2)
    for d in (-2, 2):
        signal(token.at[1], at(d, 0))

    tiles = cols // wide
    for n in range(tiles):
        there = pl.ds(n * wide, wide)
        for p in range(4):
            box = jnp.dot(band[...], planes[p, :, there], preferred_element_type=F32)
            high, low = split_pair(box[HALO:inner])
            high_in[n, p] = high
            low_in[n, p] = low
            own_edge[p, pl.ds(0, HALO), there] = box[:HALO]
            own_edge[p, pl.ds(HALO, HALO), there] = box[inner:]

    sweep_load.wait()
    along = ((my_row * rows + lane_of((LANES, rows))).astype(F32) + 0.5) * (2.0 / (rows * count_rows)) - 1.0
    burst = row_of((LANES, rows))
    power = burst // SWEEP_TALLY
    chosen = jnp.where((burst - power * SWEEP_TALLY == sweep[...]) & (power < 3), 1.0, 0.0)
    membership[1] = chosen * jnp.where(power == 0, 1.0, jnp.where(power == 1, along, along * along))
    membership[0] = jnp.transpose(jnp.where(burst == sweep[...], 1.0, 0.0))

    for copy in col_copies:
        copy.wait()
    side_exists = [jnp.where(my_col > 0, 1.0, 0.0), jnp.where(my_col < count_cols - 1, 1.0, 0.0)]
    for i, arrived in enumerate((left_in, right_in)):
        there = pl.ds(i * LANES, LANES)
        high, low = split_pair(arrived[pl.ds(HALO, rows), :] * side_exists[i])
        side_planes[pl.ds(0, rows), there] = high
        side_planes[pl.ds(rows, rows), there] = low
    side_boxed[...] = jnp.dot(band[...], side_planes[...], preferred_element_type=F32)

    def join(high_ref, low_ref, join_ref, count, side_lines):
        first_half = lane_of((count, LANES)) < LANES // 2
        parts = [high_ref, low_ref]
        for p in range(4):
            packed = side_lines()
            left = split_pair(pltpu.roll(packed[:, :LANES], LANES - SIDE * (p + 1), 1))
            right = packed[:, LANES:]
            right = split_pair(right if p == 0 else pltpu.roll(right, LANES - SIDE * p, 1))
            for n in range(tiles):
                for i in range(2):
                    before = left[i] if n == 0 else parts[i][n - 1, p, :, pl.ds(LANES, LANES)]
                    after = right[i] if n == tiles - 1 else parts[i][n + 1, p, :, pl.ds(0, LANES)]
                    join_ref[n, p, :, pl.ds(i * LANES, LANES)] = jnp.where(first_half, after, before)

    def box_across(high_ref, low_ref, join_ref, box_ref, count, n):
        lines = 4 * count
        total = jnp.dot(high_ref[n].reshape(lines, wide), across_box[...], preferred_element_type=F32)
        total += jnp.dot(low_ref[n].reshape(lines, wide), across_box[...], preferred_element_type=F32)
        total += jnp.dot(join_ref[n].reshape(lines, wide), across_join[...], preferred_element_type=F32)
        box_ref[n] = total.reshape(4, count, wide)

    between = inner - HALO
    join(high_in, low_in, join_in, between, lambda: side_boxed[pl.ds(HALO, between), :])

    for n in range(tiles):
        box_across(high_in, low_in, join_in, box_in, between, n)

    across_first = ((my_col * cols + lane).astype(F32) + 0.5) * (2.0 / (cols * count_cols)) - 1.0

    def finish(box_ref, at_row, row):
        here = pl.ds(row, 8)
        totals = [jnp.zeros((8, LANES), F32) for _ in range(7)]
        for j in range(blocks):
            half = pl.ds(j % 2 * LANES, LANES)
            real, imag, power_a, power_b = (box_ref[j // 2, p, pl.ds(at_row, 8), half] for p in range(4))
            scale = lax.rsqrt((power_a + 1.0) * (power_b + 1.0))
            real, imag = real * scale, imag * scale
            there = pl.ds(j * LANES, LANES)
            gamma[0, here, there] = real
            gamma[1, here, there] = imag
            w = weight[here, there].astype(F32)
            across = across_first + j * (LANES * 2.0 / (cols * count_cols))
            wu = w * across
            terms = (w, wu, wu * across, w * real, w * imag, wu * real, wu * imag)
            totals = [total + term for total, term in zip(totals, terms)]
        line = jnp.zeros((8, LANES), F32)
        for q, total in enumerate(totals):
            line = jnp.where(lane == q, jnp.sum(total, axis=1, keepdims=True), line)
        sums[here, :] = line

    @pl.loop(0, between // 8)
    def _(group):
        at_row = pl.multiple_of(group * 8, 8)
        finish(box_in, at_row, pl.multiple_of(at_row + HALO, 8))

    pl.semaphore_wait(token.at[1], 2)
    for d in (-4, 4):
        signal(token.at[2], at(d, 0))

    for copy in corner_copies + row_copies:
        copy.wait()
    for i, arrived in enumerate((left_in, right_in)):
        there = pl.ds(i * LANES, LANES)
        for k, to in enumerate((0, rows + HALO)):
            high, low = split_pair(arrived[pl.ds(to, HALO), :] * side_exists[i])
            corner_planes[pl.ds(2 * k * HALO, HALO), there] = high
            corner_planes[pl.ds((2 * k + 1) * HALO, HALO), there] = low
    side_edge = jnp.dot(tri[...], corner_planes[...], preferred_element_type=F32)
    side_edge += jnp.concatenate([side_boxed[pl.ds(0, HALO), :], side_boxed[pl.ds(inner, HALO), :]], axis=0)
    for p in range(4):
        for i, arrived in enumerate((above, below)):
            high, low = split_pair(arrived[p])
            halo_planes[p, pl.ds(2 * i * HALO, HALO), :] = high
            halo_planes[p, pl.ds((2 * i + 1) * HALO, HALO), :] = low
    for n in range(tiles):
        there = pl.ds(n * wide, wide)
        for p in range(4):
            extra = jnp.dot(tri[...], halo_planes[p, :, there], preferred_element_type=F32)
            high, low = split_pair(own_edge[p, :, there] + extra)
            high_edge[n, p] = high
            low_edge[n, p] = low
    join(
        high_edge, low_edge, join_edge, 2 * HALO,
        lambda: side_edge,
    )
    for n in range(tiles):
        box_across(high_edge, low_edge, join_edge, box_edge, 2 * HALO, n)
    for group in range(2 * HALO // 8):
        at_row = group * 8
        finish(box_edge, at_row, at_row if at_row < HALO else at_row - HALO + inner)

    full = lax.dot_general(
        jnp.transpose(sums[...])[:8], membership[1], (((1,), (1,)), ((), ())), preferred_element_type=F32, precision=EXACT
    )
    table[...] = full[:4] + pltpu.roll(full[4:], LANES // 2, 1)

    copies = [
        send(table, from_cols.at[k - 1], ysend.at[k - 1], yrecv.at[k - 1], at(0, k)) for k in range(1, 4)
    ]
    pl.semaphore_wait(token.at[2], 2)
    for copy in copies:
        copy.wait()
    table_rows[...] = (table[...] + from_cols[0]) + (from_cols[1] + from_cols[2])
    distances = [d for k in range(1, REACH + 1) for d in (-k, k)]
    copies = [
        send(table_rows, from_rows.at[i], rsend.at[i], rrecv.at[i], at(d, 0)) for i, d in enumerate(distances)
    ]
    for copy in copies:
        copy.wait()
    total = table_rows[...]
    for i in range(len(distances)):
        total = total + from_rows[i]

    total = jnp.concatenate([total, pltpu.roll(total, LANES // 2, 1)], axis=0)
    once = pltpu.roll(total, LANES - SWEEP_TALLY, 1)
    twice = pltpu.roll(total, LANES - 2 * SWEEP_TALLY, 1)
    count, sum_u, sum_uu, h0_re, h0_im, hu_re, hu_im = (total[q:q + 1] for q in range(7))
    sum_v, sum_uv, hv_re, hv_im = (once[q:q + 1] for q in (0, 1, 3, 4))
    sum_vv = twice[0:1]
    floored = jnp.maximum(count, 1.0)
    mean_u = sum_u / floored
    mean_v = sum_v / floored
    guu = sum_uu - 2.0 * mean_u * sum_u + mean_u * mean_u * count
    guv = sum_uv - mean_u * sum_v - mean_v * sum_u + mean_u * mean_v * count
    gvv = sum_vv - 2.0 * mean_v * sum_v + mean_v * mean_v * count
    ridge = 0.001 * count + 1.0
    diag_u = guu + ridge
    diag_v = gvv + ridge
    inverse = 1.0 / (diag_u * diag_v - guv * guv)
    base = 1.0 / (count + ridge)
    out = []
    slopes_u, slopes_v = [], []
    for h0, hu, hv in ((h0_re, hu_re, hv_re), (h0_im, hu_im, hv_im)):
        hu = hu - mean_u * h0
        hv = hv - mean_v * h0
        out.append(h0 * base)
        slopes_u.append((diag_v * hu - guv * hv) * inverse)
        slopes_v.append((diag_u * hv - guv * hu) * inverse)
    entries = out + slopes_u + slopes_v + [mean_u, mean_v]
    stacked = jnp.zeros((LANES, LANES), F32)
    place = row_of((LANES, LANES))
    for i, entry in enumerate(entries):
        stacked = jnp.where(place == i, entry, stacked)
    stacked = jnp.where(lane_of((LANES, LANES)) < SWEEP_TALLY, stacked, 0.0)
    coefs[...] = lax.dot_general(
        membership[0], stacked, (((1,), (1,)), ((), ())), preferred_element_type=F32, precision=EXACT
    )


def ramp_kernel(count_rows, count_cols, gamma, coefs, deramped, coherence, out, size, sem):
    _, rows, cols = gamma.shape
    my_row = lax.axis_index("rows")
    my_col = lax.axis_index("cols")
    lane = lane_of((8, LANES))
    across_first = ((my_col * cols + lane).astype(F32) + 0.5) * (2.0 / (cols * count_cols)) - 1.0
    chunk = 32
    copies = []
    for low in range(0, rows, chunk):
        @pl.loop(low // 8, (low + chunk) // 8)
        def _(group):
            start = pl.multiple_of(group * 8, 8)
            here = pl.ds(start, 8)
            line = coefs[here, :]
            along = ((my_row * rows + start + row_of((8, LANES))).astype(F32) + 0.5) * (
                2.0 / (rows * count_rows)
            ) - 1.0
            wide = [jnp.broadcast_to(line[:, q:q + 1], (8, LANES)) for q in range(8)]
            along = along - wide[7]
            base_re = wide[0] + wide[4] * along
            base_im = wide[1] + wide[5] * along
            centred = across_first - wide[6]
            for j in range(cols // LANES):
                there = pl.ds(j * LANES, LANES)
                du = centred + j * (LANES * 2.0 / (cols * count_cols))
                model_re = base_re + wide[2] * du
                model_im = base_im + wide[3] * du
                real, imag = gamma[0, here, there], gamma[1, here, there]
                out[0, here, there] = real * model_re + imag * model_im
                out[1, here, there] = imag * model_re - real * model_im
                size[here, there] = jnp.sqrt(real * real + imag * imag)

        here = pl.ds(low, chunk)
        for source, target in ((out.at[:, here, :], deramped.at[:, here, :]), (size.at[here, :], coherence.at[here, :])):
            copy = pltpu.make_async_copy(source, target, sem.at[len(copies)])
            copy.start()
            copies.append(copy)
    for copy in copies:
        copy.wait()


def on_device(count_rows, count_cols, lead, trail, flags, sweep):
    rows, cols = flags.shape
    tall = rows + 2 * HALO
    wide = 2 * LANES
    tiles, between = cols // wide, rows - 2 * HALO
    vmem = pl.BlockSpec(memory_space=pltpu.VMEM)
    hbm = pl.BlockSpec(memory_space=pl.ANY)
    dma = pltpu.SemaphoreType.DMA
    V = pltpu.VMEM
    gamma, coefs = pl.pallas_call(
        functools.partial(gamma_kernel, count_rows, count_cols),
        out_shape=(V((2, rows, cols), F32), V((rows, LANES), F32)),
        in_specs=[hbm, hbm, hbm, hbm],
        out_specs=(vmem, vmem),
        scratch_shapes=[
            V((2, rows, cols), F32), V((2, rows, cols), F32), V((rows, cols), jnp.int32), V((1, rows), jnp.int32),
            V((4, 2 * rows, cols), BF16),
            V((4, HALO, cols), F32), V((4, HALO, cols), F32), V((4, HALO, cols), F32), V((4, HALO, cols), F32),
            V((rows, LANES), F32), V((rows, LANES), F32), V((tall, LANES), F32), V((tall, LANES), F32),
            V((rows, 2 * LANES), F32), V((2 * rows, 2 * LANES), BF16), V((4 * HALO, 2 * LANES), BF16),
            V((rows, 2 * rows), BF16), V((2 * HALO, 4 * HALO), BF16),
            V((4, 4 * HALO, cols), BF16), V((wide, wide), BF16), V((wide, wide), BF16),
            V((tiles, 4, between, wide), BF16), V((tiles, 4, between, wide), BF16),
            V((tiles, 4, between, wide), BF16), V((tiles, 4, between, wide), F32),
            V((4, 2 * HALO, cols), F32),
            V((tiles, 4, 2 * HALO, wide), BF16), V((tiles, 4, 2 * HALO, wide), BF16),
            V((tiles, 4, 2 * HALO, wide), BF16), V((tiles, 4, 2 * HALO, wide), F32),
            V((rows, LANES), F32), V((2, LANES, rows), F32),
            V((4, LANES), F32), V((3, 4, LANES), F32), V((4, LANES), F32), V((2 * REACH, 4, LANES), F32),
            dma((22,)), dma((2,)), dma((2,)), dma((6,)), dma((6,)), dma((3,)), dma((3,)),
            dma((2 * REACH,)), dma((2 * REACH,)), pltpu.SemaphoreType.REGULAR((3,)),
        ],
        compiler_params=pltpu.CompilerParams(
            collective_id=0, has_side_effects=True, vmem_limit_bytes=64_000_000
        ),
        name="coherence",
    )(lead, trail, flags, sweep.reshape(1, rows))
    return pl.pallas_call(
        functools.partial(ramp_kernel, count_rows, count_cols),
        out_shape=(
            jax.ShapeDtypeStruct((2, rows, cols), F32),
            jax.ShapeDtypeStruct((rows, cols), F32),
        ),
        in_specs=[vmem, vmem],
        out_specs=(hbm, hbm),
        scratch_shapes=[V((2, rows, cols), F32), V((rows, cols), F32), dma((8,))],
        compiler_params=pltpu.CompilerParams(vmem_limit_bytes=16 * 1024 * 1024),
        name="ramp",
    )(gamma, coefs)


def solution(mesh):
    in_specs = (P(None, "rows", "cols"), P(None, "rows", "cols"), P("rows", "cols"), P("rows"))
    out_specs = (P(None, "rows", "cols"), P("rows", "cols"))
    body = functools.partial(on_device, mesh.shape["rows"], mesh.shape["cols"])
    return jax.shard_map(body, mesh=mesh, in_specs=in_specs, out_specs=out_specs, check_vma=False)
```

```python
import functools

import jax
import jax.numpy as jnp
from jax import lax
from jax.experimental import pallas as pl
from jax.experimental.pallas import tpu as pltpu
from jax.sharding import PartitionSpec as P

WIN_R = 32
WIN_C = 8
SWEEP_TALLY = 16
HALO = WIN_R // 2
SIDE = WIN_C // 2
LANES = 128
REACH = 8
PARTS = 4
MESH = pl.DeviceIdType.MESH
F32 = jnp.float32
BF16 = jnp.bfloat16
EXACT = lax.Precision.HIGHEST


def split_pair(x):
    high = x.astype(BF16)
    return high, (x - high.astype(F32)).astype(BF16)


def lane_of(shape):
    return lax.broadcasted_iota(jnp.int32, shape, 1)


def row_of(shape):
    return lax.broadcasted_iota(jnp.int32, shape, 0)


def gamma_kernel(
    count_rows, count_cols,
    lead, trail, flags, sweep_in,
    gamma, size, coefs,
    first, second, weight, sweep, planes, up_out, down_out, above, below, left_out, right_out, left_in, right_in,
    side_boxed, side_edge, side_planes, corner_planes, band, tri, halo_planes, across_box, across_join,
    high_in, low_in, join_in, box_in, own_edge, high_edge, low_edge, join_edge, box_edge,
    line_in, line_edge, sums, membership, table, from_cols, table_rows, from_rows,
    load_sem, row_send, row_recv, col_send, col_recv, ysend, yrecv, rsend, rrecv, token,
):
    rows, cols = weight.shape
    blocks = cols // LANES
    my_row = lax.axis_index("rows")
    my_col = lax.axis_index("cols")

    def at(d_row, d_col):
        return {
            "rows": lax.rem(my_row + d_row + count_rows, count_rows),
            "cols": lax.rem(my_col + d_col + count_cols, count_cols),
        }

    def signal(sem, where):
        pl.semaphore_signal(sem, inc=1, device_id=where, device_id_type=MESH)

    barrier = pltpu.get_barrier_semaphore()
    def exists(d_row):
        return my_row >= -d_row if d_row < 0 else my_row < count_rows - d_row

    def if_row(d_row, act):
        if d_row:
            pl.when(exists(d_row))(act)
        else:
            act()

    def number(*d_rows):
        return sum(exists(d).astype(jnp.int32) for d in d_rows)

    for a in (-1, 0, 1):
        for b in (-1, 0, 1) if a else (-1, 1, 2):
            if_row(a, lambda a=a, b=b: signal(barrier, at(a, b)))

    loads = []

    def load(low, high, left, right):
        started = []
        window = (pl.ds(low, high - low), pl.ds(left, right - left))
        for source, target in ((lead, first), (trail, second)):
            started.append((source.at[(slice(None),) + window], target.at[(slice(None),) + window]))
        started.append((flags.at[window], weight.at[window]))
        copies = []
        for source, target in started:
            copy = pltpu.make_async_copy(source, target, load_sem.at[len(loads)])
            copy.start()
            loads.append(copy)
            copies.append(copy)
        return copies

    def arrive(copies):
        for copy in copies:
            copy.wait()

    inner = rows - HALO
    part = cols // PARTS
    edge_loads = []
    for c in range(PARTS):
        right = (c + 1) * part - (LANES if c == PARTS - 1 else 0)
        edge_loads.append(load(0, HALO, c * part, right) + load(inner, rows, c * part, right))
        if c == 0:
            edge_loads[0] += load(0, HALO, cols - LANES, cols) + load(inner, rows, cols - LANES, cols)
    side_loads = load(HALO, inner, 0, LANES) + load(HALO, inner, cols - LANES, cols)
    step = (inner - HALO) // 3
    sweep_load = pltpu.make_async_copy(sweep_in, sweep, load_sem.at[len(loads)])
    sweep_load.start()
    loads.append(sweep_load)
    main_loads = [load(HALO + i * step, HALO + (i + 1) * step, LANES, cols - LANES) for i in range(3)]

    lane = lane_of((8, LANES))
    lane16 = lane_of((HALO, LANES))

    def products(row, block, sends=None):
        here = (pl.ds(row, HALO), pl.ds(block * LANES, LANES))
        w = weight[here].astype(F32)
        real_a, imag_a = first[(0,) + here] * w, first[(1,) + here] * w
        real_b, imag_b = second[(0,) + here] * w, second[(1,) + here] * w
        if sends is not None:
            top = jnp.maximum(jnp.abs(real_b), jnp.abs(imag_b))
            some = top > 0.0
            unit = 1.0 / jnp.where(some, top, 1.0)
            x, y = jnp.where(some, real_b * unit, 1.0), imag_b * unit
            square = x * x + y * y
            turn = lax.rsqrt(square)
            there = here[1]
            sends[0, :, there] = (real_a * x + imag_a * y) * turn
            sends[1, :, there] = (imag_a * x - real_a * y) * turn
            sends[2, :, there] = top * (square * turn)
        return (
            real_a * real_b + imag_a * imag_b,
            imag_a * real_b - real_a * imag_b,
            real_a * real_a + imag_a * imag_a,
            real_b * real_b + imag_b * imag_b,
        )

    def fill(row, sends=None, some=range(blocks)):
        for block in some:
            here = pl.ds(block * LANES, LANES)
            for p, x in enumerate(products(row, block, sends)):
                high, low = split_pair(x)
                planes[p, pl.ds(row, HALO), here] = high
                planes[p, pl.ds(rows + row, HALO), here] = low

    def pack(row):
        packed_left = jnp.zeros((HALO, LANES), F32)
        packed_right = jnp.zeros((HALO, LANES), F32)
        for p, x in enumerate(products(row, 0)):
            x = jnp.where(lane16 < SIDE, x, 0.0)
            packed_left += x if p == 0 else pltpu.roll(x, SIDE * p, 1)
        for p, x in enumerate(products(row, blocks - 1)):
            packed_right += pltpu.roll(jnp.where(lane16 >= LANES - SIDE, x, 0.0), SIDE * (p + 1), 1)
        left_out[pl.ds(row, HALO), :] = packed_left
        right_out[pl.ds(row, HALO), :] = packed_right

    def send(source, target, send_sem, recv_sem, d_row, d_col):
        copy = pltpu.make_async_remote_copy(
            src_ref=source, dst_ref=target, send_sem=send_sem, recv_sem=recv_sem,
            device_id=at(d_row, d_col), device_id_type=MESH,
        )
        if_row(d_row, copy.start)
        return copy, d_row

    def finish_send(sent):
        copy, d_row = sent
        if_row(-d_row, copy.wait_recv)
        if_row(d_row, copy.wait_send)

    @pl.when(my_row == 0)
    def _():
        above[...] = jnp.zeros_like(above)
        for arrived in (left_in, right_in):
            arrived[pl.ds(0, HALO), :] = jnp.zeros((HALO, LANES), F32)

    @pl.when(my_row == count_rows - 1)
    def _():
        below[...] = jnp.zeros_like(below)
        for arrived in (left_in, right_in):
            arrived[pl.ds(rows + HALO, HALO), :] = jnp.zeros((HALO, LANES), F32)

    distances = [d for k in range(REACH, 0, -1) for d in (-k, k)]
    for i, d in enumerate(distances):
        @pl.when(jnp.logical_not(exists(-d)))
        def _(i=i):
            from_rows[i] = jnp.zeros((4, LANES), F32)

    col_copies, corner_copies, row_copies = [], [], []

    def send_side(copies, source, target, low, count, to, d_row, d_col):
        i = len(col_copies) + len(corner_copies)
        copies.append(
            send(
                source.at[pl.ds(low, count), :], target.at[pl.ds(to, count), :],
                col_send.at[i], col_recv.at[i], d_row, d_col,
            )
        )

    sides = ((left_out, right_in, -1), (right_out, left_in, 1))
    for c in range(PARTS):
        arrive(edge_loads[c])
        if c == 0:
            pack(0)
            pack(inner)
        some = range(c * part // LANES, (c + 1) * part // LANES)
        fill(0, up_out, some)
        fill(inner, down_out, some)
        if c == 0:
            pl.semaphore_wait(barrier, 3 + 3 * number(-1, 1))
            for source, target, d_col in sides:
                send_side(corner_copies, source, target, 0, HALO, rows + HALO, -1, d_col)
                send_side(corner_copies, source, target, inner, HALO, 0, 1, d_col)
        there = pl.ds(c * part, part)
        row_copies.append([
            send(
                source.at[:, :, there], target.at[:, :, there],
                row_send.at[2 * c + i], row_recv.at[2 * c + i], d_row, 0,
            )
            for i, (source, target, d_row) in enumerate(((up_out, below, -1), (down_out, above, 1)))
        ])
    arrive(side_loads)
    for row in range(HALO, inner, HALO):
        pack(row)
    for source, target, d_col in sides:
        send_side(col_copies, source, target, 0, rows, HALO, 0, d_col)
    for d in (-1, 1):
        if_row(d, lambda d=d: signal(token.at[0], at(d, 0)))

    box_row = row_of((rows, 2 * rows))
    box_col = lax.rem(lane_of((rows, 2 * rows)), rows) - box_row
    band[...] = jnp.where((box_col >= -HALO) & (box_col < HALO), 1.0, 0.0).astype(BF16)
    tri_row = row_of((2 * HALO, 4 * HALO))
    tri_lane = lane_of((2 * HALO, 4 * HALO))
    tri_col = lax.rem(tri_lane, HALO)
    has_above = jnp.where(my_row > 0, 1.0, 0.0)
    has_below = jnp.where(my_row < count_rows - 1, 1.0, 0.0)
    tri_above = jnp.where((tri_row < HALO) & (tri_lane < 2 * HALO) & (tri_col >= tri_row), has_above, 0.0)
    tri_below = jnp.where((tri_row >= HALO) & (tri_lane >= 2 * HALO) & (tri_col < tri_row - HALO), has_below, 0.0)
    tri[...] = (tri_above + tri_below).astype(BF16)
    wide = 2 * LANES
    from_lane = row_of((wide, wide))
    to_lane = lane_of((wide, wide))
    apart = from_lane - to_lane
    across_box[...] = jnp.where((apart >= -SIDE) & (apart < SIDE), 1.0, 0.0).astype(BF16)
    from_lane = lax.rem(from_lane, LANES)
    before = (from_lane >= LANES - SIDE) & (to_lane <= from_lane - (LANES - SIDE))
    after = (from_lane < SIDE - 1) & (to_lane >= wide - SIDE + 1 + from_lane)
    across_join[...] = jnp.where(before | after, 1.0, 0.0).astype(BF16)

    for i, copies in enumerate(main_loads):
        arrive(copies)

        @pl.loop(HALO + i * step, HALO + (i + 1) * step, step=HALO)
        def _(row):
            fill(pl.multiple_of(row, HALO))

    tiles = cols // wide
    for n in range(tiles):
        there = pl.ds(n * wide, wide)
        for p in range(4):
            box = jnp.dot(band[...], planes[p, :, there], preferred_element_type=F32)
            high, low = split_pair(box[HALO:inner])
            high_in[n, p] = high
            low_in[n, p] = low
            own_edge[p, pl.ds(0, HALO), there] = box[:HALO]
            own_edge[p, pl.ds(HALO, HALO), there] = box[inner:]

    sweep_load.wait()
    along = ((my_row * rows + lane_of((LANES, rows))).astype(F32) + 0.5) * (2.0 / (rows * count_rows)) - 1.0
    burst = row_of((LANES, rows))
    power = burst // SWEEP_TALLY
    chosen = jnp.where((burst - power * SWEEP_TALLY == sweep[...]) & (power < 3), 1.0, 0.0)
    membership[1] = chosen * jnp.where(power == 0, 1.0, jnp.where(power == 1, along, along * along))
    membership[0] = jnp.transpose(jnp.where(burst == sweep[...], 1.0, 0.0))

    def join(high_ref, low_ref, join_ref, count, n, packed):
        first_half = lane_of((count, LANES)) < LANES // 2
        parts = [high_ref, low_ref]
        for p in range(4):
            if n == 0:
                outer = split_pair(pltpu.roll(packed[:, :LANES], LANES - SIDE * (p + 1), 1))
            elif n == tiles - 1:
                outer = packed[:, LANES:]
                outer = split_pair(outer if p == 0 else pltpu.roll(outer, LANES - SIDE * p, 1))
            for i in range(2):
                before = outer[i] if n == 0 else parts[i][n - 1, p, :, pl.ds(LANES, LANES)]
                after = outer[i] if n == tiles - 1 else parts[i][n + 1, p, :, pl.ds(0, LANES)]
                join_ref[n, p, :, pl.ds(i * LANES, LANES)] = jnp.where(first_half, after, before)

    def box_across(high_ref, low_ref, join_ref, box_ref, count, n):
        lines = 4 * count
        total = jnp.dot(high_ref[n].reshape(lines, wide), across_box[...], preferred_element_type=F32)
        total += jnp.dot(low_ref[n].reshape(lines, wide), across_box[...], preferred_element_type=F32)
        total += jnp.dot(join_ref[n].reshape(lines, wide), across_join[...], preferred_element_type=F32)
        box_ref[n] = total.reshape(4, count, wide)

    across_first = ((my_col * cols + lane).astype(F32) + 0.5) * (2.0 / (cols * count_cols)) - 1.0

    def finish(box_ref, line_ref, n, at_row, row, fresh):
        here = pl.ds(row, 8)
        totals = None if fresh else [line_ref[q, pl.ds(at_row, 8), :] for q in range(7)]
        for j in (2 * n, 2 * n + 1):
            half = pl.ds(j % 2 * LANES, LANES)
            real, imag, power_a, power_b = (box_ref[n, p, pl.ds(at_row, 8), half] for p in range(4))
            scale = lax.rsqrt((power_a + 1.0) * (power_b + 1.0))
            real, imag = real * scale, imag * scale
            there = pl.ds(j * LANES, LANES)
            gamma[0, here, there] = real
            gamma[1, here, there] = imag
            w = weight[here, there].astype(F32)
            across = across_first + j * (LANES * 2.0 / (cols * count_cols))
            wu = w * across
            terms = (w, wu, wu * across, w * real, w * imag, wu * real, wu * imag)
            totals = list(terms) if totals is None else [total + term for total, term in zip(totals, terms)]
        for q, total in enumerate(totals):
            line_ref[q, pl.ds(at_row, 8), :] = total

    def gather_lines(line_ref, at_row, row):
        line = jnp.zeros((8, LANES), F32)
        for q in range(7):
            line = jnp.where(lane == q, jnp.sum(line_ref[q, pl.ds(at_row, 8), :], axis=1, keepdims=True), line)
        sums[pl.ds(row, 8), :] = line

    between = inner - HALO

    def run_inner(order, fresh_at, packed=None):
        waiting = None
        for n in order + [None]:
            if n is not None:
                join(high_in, low_in, join_in, between, n, packed)
                box_across(high_in, low_in, join_in, box_in, between, n)
            if waiting is not None:
                for at_row in range(0, between, 8):
                    finish(box_in, line_in, waiting, at_row, at_row + HALO, waiting == fresh_at)
            waiting = n

    run_inner(list(range(1, tiles - 1)), 1)

    pl.semaphore_wait(token.at[0], number(-1, 1))
    for d in (-2, 2):
        if_row(d, lambda d=d: signal(token.at[1], at(d, 0)))

    for sent in col_copies:
        finish_send(sent)
    side_exists = [jnp.where(my_col > 0, 1.0, 0.0), jnp.where(my_col < count_cols - 1, 1.0, 0.0)]
    for i, arrived in enumerate((left_in, right_in)):
        there = pl.ds(i * LANES, LANES)
        high, low = split_pair(arrived[pl.ds(HALO, rows), :] * side_exists[i])
        side_planes[pl.ds(0, rows), there] = high
        side_planes[pl.ds(rows, rows), there] = low
    side_boxed[...] = jnp.dot(band[...], side_planes[...], preferred_element_type=F32)
    run_inner([0, tiles - 1], None, side_boxed[pl.ds(HALO, between), :])
    for at_row in range(0, between, 8):
        gather_lines(line_in, at_row, at_row + HALO)

    for sent in corner_copies:
        finish_send(sent)
    for i, arrived in enumerate((left_in, right_in)):
        there = pl.ds(i * LANES, LANES)
        for k, to in enumerate((0, rows + HALO)):
            high, low = split_pair(arrived[pl.ds(to, HALO), :] * side_exists[i])
            corner_planes[pl.ds(2 * k * HALO, HALO), there] = high
            corner_planes[pl.ds((2 * k + 1) * HALO, HALO), there] = low
    side_edge[...] = jnp.dot(tri[...], corner_planes[...], preferred_element_type=F32) + jnp.concatenate(
        [side_boxed[pl.ds(0, HALO), :], side_boxed[pl.ds(inner, HALO), :]], axis=0
    )

    ready = 0
    for c in range(PARTS):
        for sent in row_copies[c]:
            finish_send(sent)
        if c == 0:
            pl.semaphore_wait(token.at[1], number(-2, 2))
            for d in (-4, 4):
                if_row(d, lambda d=d: signal(token.at[2], at(d, 0)))
        here = pl.ds(c * part, part)
        for i, arrived in enumerate((above, below)):
            turned_re, turned_im, length = (arrived[q, :, here] for q in range(3))
            arrived_planes = (
                turned_re * length, turned_im * length, turned_re * turned_re + turned_im * turned_im, length * length
            )
            for p, x in enumerate(arrived_planes):
                high, low = split_pair(x)
                halo_planes[p, pl.ds(2 * i * HALO, HALO), here] = high
                halo_planes[p, pl.ds((2 * i + 1) * HALO, HALO), here] = low
        last = (c + 1) * part // wide
        for n in range(c * part // wide, last):
            there = pl.ds(n * wide, wide)
            for p in range(4):
                extra = jnp.dot(tri[...], halo_planes[p, :, there], preferred_element_type=F32)
                high, low = split_pair(own_edge[p, :, there] + extra)
                high_edge[n, p] = high
                low_edge[n, p] = low
        until = last if last == tiles else last - 1
        for n in range(ready, until):
            join(high_edge, low_edge, join_edge, 2 * HALO, n, side_edge[...])
            box_across(high_edge, low_edge, join_edge, box_edge, 2 * HALO, n)
        for n in range(ready, until):
            for at_row in range(0, 2 * HALO, 8):
                finish(box_edge, line_edge, n, at_row, at_row if at_row < HALO else at_row - HALO + inner, n == 0)
        ready = until
    for at_row in range(0, 2 * HALO, 8):
        gather_lines(line_edge, at_row, at_row if at_row < HALO else at_row - HALO + inner)

    full = lax.dot_general(
        jnp.transpose(sums[...])[:8], membership[1], (((1,), (1,)), ((), ())), preferred_element_type=F32, precision=EXACT
    )
    table[...] = full[:4] + pltpu.roll(full[4:], LANES // 2, 1)

    copies = [
        send(table, from_cols.at[k - 1], ysend.at[k - 1], yrecv.at[k - 1], 0, k) for k in (2, 1, 3)
    ]
    pl.semaphore_wait(token.at[2], number(-4, 4))
    for sent in copies:
        finish_send(sent)
    table_rows[...] = (table[...] + from_cols[0]) + (from_cols[1] + from_cols[2])
    copies = [
        send(table_rows, from_rows.at[i], rsend.at[i], rrecv.at[i], d, 0) for i, d in enumerate(distances)
    ]

    @pl.loop(0, rows // 8)
    def _(group):
        here = pl.ds(pl.multiple_of(group * 8, 8), 8)
        for j in range(blocks):
            there = pl.ds(j * LANES, LANES)
            real, imag = gamma[0, here, there], gamma[1, here, there]
            size[here, there] = jnp.sqrt(real * real + imag * imag)

    for sent in copies:
        finish_send(sent)
    total = table_rows[...]
    for i in range(len(distances)):
        total = total + from_rows[i]

    total = jnp.concatenate([total, pltpu.roll(total, LANES // 2, 1)], axis=0)
    once = pltpu.roll(total, LANES - SWEEP_TALLY, 1)
    twice = pltpu.roll(total, LANES - 2 * SWEEP_TALLY, 1)
    count, sum_u, sum_uu, h0_re, h0_im, hu_re, hu_im = (total[q:q + 1] for q in range(7))
    sum_v, sum_uv, hv_re, hv_im = (once[q:q + 1] for q in (0, 1, 3, 4))
    sum_vv = twice[0:1]
    floored = jnp.maximum(count, 1.0)
    mean_u = sum_u / floored
    mean_v = sum_v / floored
    guu = sum_uu - 2.0 * mean_u * sum_u + mean_u * mean_u * count
    guv = sum_uv - mean_u * sum_v - mean_v * sum_u + mean_u * mean_v * count
    gvv = sum_vv - 2.0 * mean_v * sum_v + mean_v * mean_v * count
    ridge = 0.001 * count + 1.0
    diag_u = guu + ridge
    diag_v = gvv + ridge
    inverse = 1.0 / (diag_u * diag_v - guv * guv)
    base = 1.0 / (count + ridge)
    out = []
    slopes_u, slopes_v = [], []
    for h0, hu, hv in ((h0_re, hu_re, hv_re), (h0_im, hu_im, hv_im)):
        hu = hu - mean_u * h0
        hv = hv - mean_v * h0
        out.append(h0 * base)
        slopes_u.append((diag_v * hu - guv * hv) * inverse)
        slopes_v.append((diag_u * hv - guv * hu) * inverse)
    entries = out + slopes_u + slopes_v + [mean_u, mean_v]
    stacked = jnp.zeros((LANES, LANES), F32)
    place = row_of((LANES, LANES))
    for i, entry in enumerate(entries):
        stacked = jnp.where(place == i, entry, stacked)
    stacked = jnp.where(lane_of((LANES, LANES)) < SWEEP_TALLY, stacked, 0.0)
    coefs[...] = lax.dot_general(
        membership[0], stacked, (((1,), (1,)), ((), ())), preferred_element_type=F32, precision=EXACT
    )


def ramp_kernel(count_rows, count_cols, gamma, size, coefs, deramped, coherence, out, sem):
    _, rows, cols = gamma.shape
    my_row = lax.axis_index("rows")
    my_col = lax.axis_index("cols")
    lane = lane_of((8, LANES))
    across_first = ((my_col * cols + lane).astype(F32) + 0.5) * (2.0 / (cols * count_cols)) - 1.0
    chunk = 16
    copies = [pltpu.make_async_copy(size, coherence, sem.at[0])]
    copies[0].start()
    for low in range(0, rows, chunk):
        @pl.loop(low // 8, (low + chunk) // 8)
        def _(group):
            start = pl.multiple_of(group * 8, 8)
            here = pl.ds(start, 8)
            line = coefs[here, :]
            along = ((my_row * rows + start + row_of((8, LANES))).astype(F32) + 0.5) * (
                2.0 / (rows * count_rows)
            ) - 1.0
            wide = [jnp.broadcast_to(line[:, q:q + 1], (8, LANES)) for q in range(8)]
            along = along - wide[7]
            base_re = wide[0] + wide[4] * along
            base_im = wide[1] + wide[5] * along
            centred = across_first - wide[6]
            for j in range(cols // LANES):
                there = pl.ds(j * LANES, LANES)
                du = centred + j * (LANES * 2.0 / (cols * count_cols))
                model_re = base_re + wide[2] * du
                model_im = base_im + wide[3] * du
                real, imag = gamma[0, here, there], gamma[1, here, there]
                out[0, here, there] = real * model_re + imag * model_im
                out[1, here, there] = imag * model_re - real * model_im

        here = pl.ds(low, chunk)
        copy = pltpu.make_async_copy(out.at[:, here, :], deramped.at[:, here, :], sem.at[len(copies)])
        copy.start()
        copies.append(copy)
    for copy in copies:
        copy.wait()


def on_device(count_rows, count_cols, lead, trail, flags, sweep):
    rows, cols = flags.shape
    tall = rows + 2 * HALO
    wide = 2 * LANES
    tiles, between = cols // wide, rows - 2 * HALO
    vmem = pl.BlockSpec(memory_space=pltpu.VMEM)
    hbm = pl.BlockSpec(memory_space=pl.ANY)
    dma = pltpu.SemaphoreType.DMA
    V = pltpu.VMEM
    gamma, size, coefs = pl.pallas_call(
        functools.partial(gamma_kernel, count_rows, count_cols),
        out_shape=(V((2, rows, cols), F32), V((rows, cols), F32), V((rows, LANES), F32)),
        in_specs=[hbm, hbm, hbm, hbm],
        out_specs=(vmem, vmem, vmem),
        scratch_shapes=[
            V((2, rows, cols), F32), V((2, rows, cols), F32), V((rows, cols), jnp.int32), V((1, rows), jnp.int32),
            V((4, 2 * rows, cols), BF16),
            V((3, HALO, cols), F32), V((3, HALO, cols), F32), V((3, HALO, cols), F32), V((3, HALO, cols), F32),
            V((rows, LANES), F32), V((rows, LANES), F32), V((tall, LANES), F32), V((tall, LANES), F32),
            V((rows, 2 * LANES), F32), V((2 * HALO, 2 * LANES), F32), V((2 * rows, 2 * LANES), BF16), V((4 * HALO, 2 * LANES), BF16),
            V((rows, 2 * rows), BF16), V((2 * HALO, 4 * HALO), BF16),
            V((4, 4 * HALO, cols), BF16), V((wide, wide), BF16), V((wide, wide), BF16),
            V((tiles, 4, between, wide), BF16), V((tiles, 4, between, wide), BF16),
            V((tiles, 4, between, wide), BF16), V((tiles, 4, between, wide), F32),
            V((4, 2 * HALO, cols), F32),
            V((tiles, 4, 2 * HALO, wide), BF16), V((tiles, 4, 2 * HALO, wide), BF16),
            V((tiles, 4, 2 * HALO, wide), BF16), V((tiles, 4, 2 * HALO, wide), F32),
            V((7, between, LANES), F32), V((7, 2 * HALO, LANES), F32),
            V((rows, LANES), F32), V((2, LANES, rows), F32),
            V((4, LANES), F32), V((3, 4, LANES), F32), V((4, LANES), F32), V((2 * REACH, 4, LANES), F32),
            dma((64,)), dma((2 * PARTS,)), dma((2 * PARTS,)), dma((6,)), dma((6,)), dma((3,)), dma((3,)),
            dma((2 * REACH,)), dma((2 * REACH,)), pltpu.SemaphoreType.REGULAR((3,)),
        ],
        compiler_params=pltpu.CompilerParams(
            collective_id=0, has_side_effects=True, vmem_limit_bytes=63_000_000
        ),
        name="coherence",
    )(lead, trail, flags, sweep.reshape(1, rows))
    return pl.pallas_call(
        functools.partial(ramp_kernel, count_rows, count_cols),
        out_shape=(
            jax.ShapeDtypeStruct((2, rows, cols), F32),
            jax.ShapeDtypeStruct((rows, cols), F32),
        ),
        in_specs=[vmem, vmem, vmem],
        out_specs=(hbm, hbm),
        scratch_shapes=[V((2, rows, cols), F32), dma((9,))],
        compiler_params=pltpu.CompilerParams(vmem_limit_bytes=16 * 1024 * 1024),
        name="ramp",
    )(gamma, size, coefs)


def solution(mesh):
    in_specs = (P(None, "rows", "cols"), P(None, "rows", "cols"), P("rows", "cols"), P("rows"))
    out_specs = (P(None, "rows", "cols"), P("rows", "cols"))
    body = functools.partial(on_device, mesh.shape["rows"], mesh.shape["cols"])
    return jax.shard_map(body, mesh=mesh, in_specs=in_specs, out_specs=out_specs, check_vma=False)
```

```python
import functools

import jax
import jax.numpy as jnp
from jax import lax
from jax.experimental import pallas as pl
from jax.experimental.pallas import tpu as pltpu
from jax.sharding import PartitionSpec as P

WIN_R = 32
WIN_C = 8
SWEEP_TALLY = 16
HALO = WIN_R // 2
SIDE = WIN_C // 2
LANES = 128
REACH = 8
PARTS = 4
MESH = pl.DeviceIdType.MESH
F32 = jnp.float32
BF16 = jnp.bfloat16


def split_pair(x):
    high = x.astype(BF16)
    return high, (x - high.astype(F32)).astype(BF16)


def split_three(x):
    high, rest = x.astype(BF16), x - x.astype(BF16).astype(F32)
    return high, rest.astype(BF16), (rest - rest.astype(BF16).astype(F32)).astype(BF16)


def across_lanes(x, y):
    return lax.dot_general(x, y, (((1,), (1,)), ((), ())), preferred_element_type=F32)


def lane_of(shape):
    return lax.broadcasted_iota(jnp.int32, shape, 1)


def row_of(shape):
    return lax.broadcasted_iota(jnp.int32, shape, 0)


def gamma_kernel(
    count_rows, count_cols,
    lead, trail, flags, sweep_in,
    gamma, size, coefs,
    first, second, weight, sweep, planes, up_out, down_out, above, below, side_out, side_in, corner_in,
    side_boxed, side_edge, side_planes, corner_planes, band, tri, halo_planes, across_box, across_join,
    high_in, low_in, join_in, box_in, own_edge, high_edge, low_edge, join_edge, box_edge,
    line_in, line_edge, sums, membership, table, from_cols, table_rows, from_rows,
    load_sem, row_send, row_recv, col_send, col_recv, ysend, yrecv, rsend, rrecv, token,
):
    rows, cols = weight.shape
    blocks = cols // LANES
    my_row = lax.axis_index("rows")
    my_col = lax.axis_index("cols")

    def at(d_row, d_col):
        return {
            "rows": lax.rem(my_row + d_row + count_rows, count_rows),
            "cols": lax.rem(my_col + d_col + count_cols, count_cols),
        }

    def signal(sem, where):
        pl.semaphore_signal(sem, inc=1, device_id=where, device_id_type=MESH)

    barrier = pltpu.get_barrier_semaphore()
    def exists(d_row, d_col=0):
        here, count, d = (my_row, count_rows, d_row) if d_row else (my_col, count_cols, d_col)
        return here >= -d if d < 0 else here < count - d

    def if_there(d_row, d_col, act):
        pl.when(exists(d_row, d_col))(act)

    def tell(sem, distance, along_rows):
        for d in (-distance, distance):
            where = (d, 0) if along_rows else (0, d)
            if_there(*where, lambda where=where: signal(sem, at(*where)))

    def number(distance, along_rows):
        return sum(exists(*((d, 0) if along_rows else (0, d))).astype(jnp.int32) for d in (-distance, distance))

    def hear(sem, distance, along_rows):
        pl.semaphore_wait(sem, number(distance, along_rows))

    tell(barrier, 1, True)
    tell(barrier, 1, False)

    loads = []

    def load(low, high, left, right):
        started = []
        window = (pl.ds(low, high - low), pl.ds(left, right - left))
        for source, target in ((lead, first), (trail, second)):
            started.append((source.at[(slice(None),) + window], target.at[(slice(None),) + window]))
        started.append((flags.at[window], weight.at[window]))
        copies = []
        for source, target in started:
            copy = pltpu.make_async_copy(source, target, load_sem.at[len(loads)])
            copy.start()
            loads.append(copy)
            copies.append(copy)
        return copies

    def arrive(copies):
        for copy in copies:
            copy.wait()

    inner = rows - HALO
    part = cols // PARTS
    edge_loads = []
    sweep_load = pltpu.make_async_copy(sweep_in, sweep, load_sem.at[len(loads)])
    sweep_load.start()
    loads.append(sweep_load)
    for c in range(PARTS):
        right = (c + 1) * part - (LANES if c == PARTS - 1 else 0)
        edge_loads.append(load(0, HALO, c * part, right) + load(inner, rows, c * part, right))
        if c == 0:
            edge_loads[0] += load(0, HALO, cols - LANES, cols) + load(inner, rows, cols - LANES, cols)
    side_loads = load(HALO, inner, 0, LANES) + load(HALO, inner, cols - LANES, cols)
    step = (inner - HALO) // 3
    main_loads = [load(HALO + i * step, HALO + (i + 1) * step, LANES, cols - LANES) for i in range(3)]

    lane = lane_of((8, LANES))
    lane16 = lane_of((HALO, LANES))

    def products(row, block, sends=None):
        here = (pl.ds(row, HALO), pl.ds(block * LANES, LANES))
        w = weight[here].astype(F32)
        real_a, imag_a = first[(0,) + here] * w, first[(1,) + here] * w
        real_b, imag_b = second[(0,) + here], second[(1,) + here]
        power_b = (real_b * real_b + imag_b * imag_b) * w
        if sends is not None:
            real_b, imag_b = real_b * w, imag_b * w
            top = jnp.maximum(jnp.abs(real_b), jnp.abs(imag_b))
            some = top > 0.0
            unit = 1.0 / jnp.where(some, top, 1.0)
            x, y = jnp.where(some, real_b * unit, 1.0), imag_b * unit
            square = x * x + y * y
            turn = lax.rsqrt(square)
            there = here[1]
            sends[0, :, there] = (real_a * x + imag_a * y) * turn
            sends[1, :, there] = (imag_a * x - real_a * y) * turn
            sends[2, :, there] = top * (square * turn)
        return (
            real_a * real_b + imag_a * imag_b,
            imag_a * real_b - real_a * imag_b,
            real_a * real_a + imag_a * imag_a,
            power_b,
        )

    def fill(row, sends=None, some=range(blocks)):
        for block in some:
            here = pl.ds(block * LANES, LANES)
            for p, x in enumerate(products(row, block, sends)):
                high, low = split_pair(x)
                planes[p, pl.ds(row, HALO), here] = high
                planes[p, pl.ds(rows + row, HALO), here] = low

    groups = rows // HALO
    slot = LANES // groups

    def pack(group):
        packed = [jnp.zeros((HALO, LANES), F32) for _ in range(2)]
        for p, x in enumerate(products(group * HALO, 0)):
            x = jnp.where(lane16 < SIDE, x, 0.0)
            packed[0] += x if p == 0 else pltpu.roll(x, SIDE * p, 1)
        for p, x in enumerate(products(group * HALO, blocks - 1)):
            packed[1] += pltpu.roll(jnp.where(lane16 >= LANES - SIDE, x, 0.0), SIDE * (p + 1), 1)
        return packed

    def at_slot(x, group):
        return pltpu.roll(x, slot * group, 1) if group else x

    def send(source, target, send_sem, recv_sem, d_row, d_col, ring=False):
        copy = pltpu.make_async_remote_copy(
            src_ref=source, dst_ref=target, send_sem=send_sem, recv_sem=recv_sem,
            device_id=at(d_row, d_col), device_id_type=MESH,
        )
        if ring:
            copy.start()
        else:
            if_there(d_row, d_col, copy.start)
        return copy, d_row, d_col, ring

    def finish_send(sent):
        copy, d_row, d_col, ring = sent
        if ring:
            copy.wait()
        else:
            if_there(-d_row, -d_col, copy.wait_recv)
            if_there(d_row, d_col, copy.wait_send)

    @pl.when(my_row == 0)
    def _():
        above[...] = jnp.zeros_like(above)
        corner_in[0] = jnp.zeros((2, HALO, LANES), F32)

    @pl.when(my_row == count_rows - 1)
    def _():
        below[...] = jnp.zeros_like(below)
        corner_in[1] = jnp.zeros((2, HALO, LANES), F32)

    for side, missing in enumerate((my_col == 0, my_col == count_cols - 1)):
        @pl.when(missing)
        def _(side=side):
            side_in[side] = jnp.zeros((HALO, LANES), F32)

    distances = [d for k in range(REACH, 0, -1) for d in (-k, k)]
    for i, d in enumerate(distances):
        @pl.when(jnp.logical_not(exists(-d)))
        def _(i=i):
            from_rows[i] = jnp.zeros((4, LANES), F32)

    col_copies, row_copies = [], []

    box_row = row_of((rows, 2 * rows))
    box_col = lax.rem(lane_of((rows, 2 * rows)), rows) - box_row
    band[...] = jnp.where((box_col >= -HALO) & (box_col < HALO), 1.0, 0.0).astype(BF16)
    tri_row = row_of((2 * HALO, 4 * HALO))
    tri_lane = lane_of((2 * HALO, 4 * HALO))
    tri_col = lax.rem(tri_lane, HALO)
    has_above = jnp.where(my_row > 0, 1.0, 0.0)
    has_below = jnp.where(my_row < count_rows - 1, 1.0, 0.0)
    tri_above = jnp.where((tri_row < HALO) & (tri_lane < 2 * HALO) & (tri_col >= tri_row), has_above, 0.0)
    tri_below = jnp.where((tri_row >= HALO) & (tri_lane >= 2 * HALO) & (tri_col < tri_row - HALO), has_below, 0.0)
    tri[...] = (tri_above + tri_below).astype(BF16)
    wide = 2 * LANES
    from_lane = row_of((wide, wide))
    to_lane = lane_of((wide, wide))
    apart = from_lane - to_lane
    across_box[...] = jnp.where((apart >= -SIDE) & (apart < SIDE), 1.0, 0.0).astype(BF16)
    from_lane = lax.rem(from_lane, LANES)
    before = (from_lane >= LANES - SIDE) & (to_lane <= from_lane - (LANES - SIDE))
    after = (from_lane < SIDE - 1) & (to_lane >= wide - SIDE + 1 + from_lane)
    across_join[...] = jnp.where(before | after, 1.0, 0.0).astype(BF16)

    def fill_edges(c):
        arrive(edge_loads[c])
        some = range(c * part // LANES, (c + 1) * part // LANES)
        fill(0, up_out, some)
        fill(inner, down_out, some)

    def send_edges(c):
        there = pl.ds(c * part, part)
        row_copies.append([
            send(
                source.at[:, :, there], target.at[:, :, there],
                row_send.at[2 * c + i], row_recv.at[2 * c + i], d_row, 0,
            )
            for i, (source, target, d_row) in enumerate(((up_out, below, -1), (down_out, above, 1)))
        ])

    fill_edges(0)
    ends = [pack(0), pack(groups - 1)]
    fill_edges(1)
    arrive(side_loads)
    middle = [pack(group) for group in range(1, groups - 1)]
    for side in range(2):
        side_out[side] = sum(
            (at_slot(x[side], group) for group, x in enumerate(middle + ends[1:], 1)), ends[0][side]
        )
    pl.semaphore_wait(barrier, number(1, True) + number(1, False))
    send_edges(0)
    send_edges(1)
    for side, d_col in enumerate((-1, 1)):
        col_copies.append(
            send(side_out.at[side], side_in.at[1 - side], col_send.at[side], col_recv.at[side], 0, d_col)
        )
    for c in range(2, PARTS):
        fill_edges(c)
        send_edges(c)
    tell(token.at[0], 1, True)
    tell(token.at[3], 1, False)

    sweep_load.wait()
    along = ((my_row * rows + lane_of((LANES, rows))).astype(F32) + 0.5) * (2.0 / (rows * count_rows)) - 1.0
    burst = row_of((LANES, rows))
    power = burst // SWEEP_TALLY
    chosen = jnp.where((burst - power * SWEEP_TALLY == sweep[...]) & (power < 3), 1.0, 0.0)
    for i, x in enumerate(split_three(chosen * jnp.where(power == 0, 1.0, jnp.where(power == 1, along, along * along)))):
        membership[i] = x
    membership[3] = jnp.transpose(jnp.where(burst == sweep[...], 1.0, 0.0)).astype(BF16)

    for i, copies in enumerate(main_loads):
        arrive(copies)

        @pl.loop(HALO + i * step, HALO + (i + 1) * step, step=HALO)
        def _(row):
            fill(pl.multiple_of(row, HALO))

    tiles = cols // wide
    for n in range(tiles):
        there = pl.ds(n * wide, wide)
        for p in range(4):
            box = jnp.dot(band[...], planes[p, :, there], preferred_element_type=F32)
            high, low = split_pair(box[HALO:inner])
            high_in[n, p] = high
            low_in[n, p] = low
            own_edge[p, pl.ds(0, HALO), there] = box[:HALO]
            own_edge[p, pl.ds(HALO, HALO), there] = box[inner:]

    def join(high_ref, low_ref, join_ref, count, n, packed):
        first_half = lane_of((count, LANES)) < LANES // 2
        parts = [high_ref, low_ref]
        for p in range(4):
            if n == 0:
                outer = split_pair(pltpu.roll(packed[:, :LANES], LANES - SIDE * (p + 1), 1))
            elif n == tiles - 1:
                outer = packed[:, LANES:]
                outer = split_pair(outer if p == 0 else pltpu.roll(outer, LANES - SIDE * p, 1))
            for i in range(2):
                before = outer[i] if n == 0 else parts[i][n - 1, p, :, pl.ds(LANES, LANES)]
                after = outer[i] if n == tiles - 1 else parts[i][n + 1, p, :, pl.ds(0, LANES)]
                join_ref[n, p, :, pl.ds(i * LANES, LANES)] = jnp.where(first_half, after, before)

    def box_across(high_ref, low_ref, join_ref, box_ref, count, n):
        lines = 4 * count
        total = jnp.dot(high_ref[n].reshape(lines, wide), across_box[...], preferred_element_type=F32)
        total += jnp.dot(low_ref[n].reshape(lines, wide), across_box[...], preferred_element_type=F32)
        total += jnp.dot(join_ref[n].reshape(lines, wide), across_join[...], preferred_element_type=F32)
        box_ref[n] = total.reshape(4, count, wide)

    across_first = ((my_col * cols + lane).astype(F32) + 0.5) * (2.0 / (cols * count_cols)) - 1.0

    def finish(box_ref, line_ref, n, at_row, row, fresh):
        here = pl.ds(row, 8)
        totals = None if fresh else [line_ref[q, pl.ds(at_row, 8), :] for q in range(7)]
        for j in (2 * n, 2 * n + 1):
            half = pl.ds(j % 2 * LANES, LANES)
            real, imag, power_a, power_b = (box_ref[n, p, pl.ds(at_row, 8), half] for p in range(4))
            scale = lax.rsqrt((power_a + 1.0) * (power_b + 1.0))
            real, imag = real * scale, imag * scale
            there = pl.ds(j * LANES, LANES)
            gamma[0, here, there] = real
            gamma[1, here, there] = imag
            w = weight[here, there].astype(F32)
            across = across_first + j * (LANES * 2.0 / (cols * count_cols))
            wu = w * across
            terms = (w, wu, wu * across, w * real, w * imag, wu * real, wu * imag)
            totals = list(terms) if totals is None else [total + term for total, term in zip(totals, terms)]
        for q, total in enumerate(totals):
            line_ref[q, pl.ds(at_row, 8), :] = total

    def gather_lines(line_ref, at_row, row):
        line = jnp.zeros((8, LANES), F32)
        for q in range(7):
            line = jnp.where(lane == q, jnp.sum(line_ref[q, pl.ds(at_row, 8), :], axis=1, keepdims=True), line)
        sums[pl.ds(row, 8), :] = line

    between = inner - HALO

    def run_inner(order, fresh_at, packed=None):
        waiting = None
        for n in order + [None]:
            if n is not None:
                join(high_in, low_in, join_in, between, n, packed)
                box_across(high_in, low_in, join_in, box_in, between, n)
            if waiting is not None:
                for at_row in range(0, between, 8):
                    finish(box_in, line_in, waiting, at_row, at_row + HALO, waiting == fresh_at)
            waiting = n

    run_inner(list(range(1, tiles - 1)), 1)

    hear(token.at[0], 1, True)
    tell(token.at[1], 2, True)
    hear(token.at[3], 1, False)
    tell(token.at[4], 2, False)

    for sent in col_copies:
        finish_send(sent)
    corner_copies = [
        send(side_in, corner_in.at[1 - k], col_send.at[2 + k], col_recv.at[2 + k], d_row, 0)
        for k, d_row in enumerate((-1, 1))
    ]
    side_exists = [jnp.where(my_col > 0, 1.0, 0.0), jnp.where(my_col < count_cols - 1, 1.0, 0.0)]
    for i in range(2):
        there = pl.ds(i * LANES, LANES)
        arrived = side_in[i] * side_exists[i]
        for group in range(groups):
            high, low = split_pair(pltpu.roll(arrived, LANES - slot * group, 1) if group else arrived)
            side_planes[pl.ds(group * HALO, HALO), there] = high
            side_planes[pl.ds(rows + group * HALO, HALO), there] = low
    side_boxed[...] = jnp.dot(band[...], side_planes[...], preferred_element_type=F32)
    run_inner([0, tiles - 1], None, side_boxed[pl.ds(HALO, between), :])
    for at_row in range(0, between, 8):
        gather_lines(line_in, at_row, at_row + HALO)

    for group in ((0, 1), (2,), (3,)):
        for c in group:
            for sent in row_copies[c]:
                finish_send(sent)
        start, last = group[0] * part // wide, (group[-1] + 1) * part // wide
        here = pl.ds(start * wide, (last - start) * wide)
        for i, arrived in enumerate((above, below)):
            turned_re, turned_im, length = (arrived[q, :, here] for q in range(3))
            arrived_planes = (
                turned_re * length, turned_im * length, turned_re * turned_re + turned_im * turned_im, length * length
            )
            for p, x in enumerate(arrived_planes):
                high, low = split_pair(x)
                halo_planes[p, pl.ds(2 * i * HALO, HALO), here] = high
                halo_planes[p, pl.ds((2 * i + 1) * HALO, HALO), here] = low
        for n in range(start, last):
            there = pl.ds(n * wide, wide)
            for p in range(4):
                extra = jnp.dot(tri[...], halo_planes[p, :, there], preferred_element_type=F32)
                high, low = split_pair(own_edge[p, :, there] + extra)
                high_edge[n, p] = high
                low_edge[n, p] = low
        if last == tiles:
            for sent in corner_copies:
                finish_send(sent)
            for i in range(2):
                there = pl.ds(i * LANES, LANES)
                for k in range(2):
                    arrived = corner_in[k, i] * side_exists[i]
                    high, low = split_pair(arrived if k else pltpu.roll(arrived, slot, 1))
                    corner_planes[pl.ds(2 * k * HALO, HALO), there] = high
                    corner_planes[pl.ds((2 * k + 1) * HALO, HALO), there] = low
            side_edge[...] = jnp.dot(tri[...], corner_planes[...], preferred_element_type=F32) + jnp.concatenate(
                [side_boxed[pl.ds(0, HALO), :], side_boxed[pl.ds(inner, HALO), :]], axis=0
            )
        ends_at = list(range(max(start - 1, 1), last - 1)) + ([tiles - 1, 0] if last == tiles else [])
        for n in ends_at:
            join(high_edge, low_edge, join_edge, 2 * HALO, n, side_edge[...] if last == tiles else None)
            box_across(high_edge, low_edge, join_edge, box_edge, 2 * HALO, n)
        for n in ends_at:
            for at_row in range(0, 2 * HALO, 8):
                finish(box_edge, line_edge, n, at_row, at_row if at_row < HALO else at_row - HALO + inner, n == 1)
    hear(token.at[1], 2, True)
    tell(token.at[2], 4, True)
    for at_row in range(0, 2 * HALO, 8):
        gather_lines(line_edge, at_row, at_row if at_row < HALO else at_row - HALO + inner)

    lines = split_three(jnp.transpose(sums[...])[:16])
    full = sum(across_lanes(lines[i], membership[j]) for i, j in ((2, 0), (0, 2), (1, 1), (1, 0), (0, 1), (0, 0)))[:8]
    table[...] = full[:4] + pltpu.roll(full[4:], LANES // 2, 1)

    hear(token.at[4], 2, False)
    copies = [
        send(table, from_cols.at[k - 1], ysend.at[k - 1], yrecv.at[k - 1], 0, k, True) for k in (2, 1, 3)
    ]
    hear(token.at[2], 4, True)
    for sent in copies:
        finish_send(sent)
    table_rows[...] = (table[...] + from_cols[0]) + (from_cols[1] + from_cols[2])
    copies = [
        send(table_rows, from_rows.at[i], rsend.at[i], rrecv.at[i], d, 0) for i, d in enumerate(distances)
    ]

    @pl.loop(0, rows // 8)
    def _(group):
        here = pl.ds(pl.multiple_of(group * 8, 8), 8)
        for j in range(blocks):
            there = pl.ds(j * LANES, LANES)
            real, imag = gamma[0, here, there], gamma[1, here, there]
            size[here, there] = jnp.sqrt(real * real + imag * imag)

    for sent in copies:
        finish_send(sent)
    total = table_rows[...]
    for i in range(len(distances)):
        total = total + from_rows[i]

    total = jnp.concatenate([total, pltpu.roll(total, LANES // 2, 1)], axis=0)
    once = pltpu.roll(total, LANES - SWEEP_TALLY, 1)
    twice = pltpu.roll(total, LANES - 2 * SWEEP_TALLY, 1)
    count, sum_u, sum_uu, h0_re, h0_im, hu_re, hu_im = (total[q:q + 1] for q in range(7))
    sum_v, sum_uv, hv_re, hv_im = (once[q:q + 1] for q in (0, 1, 3, 4))
    sum_vv = twice[0:1]
    floored = jnp.maximum(count, 1.0)
    mean_u = sum_u / floored
    mean_v = sum_v / floored
    guu = sum_uu - 2.0 * mean_u * sum_u + mean_u * mean_u * count
    guv = sum_uv - mean_u * sum_v - mean_v * sum_u + mean_u * mean_v * count
    gvv = sum_vv - 2.0 * mean_v * sum_v + mean_v * mean_v * count
    ridge = 0.001 * count + 1.0
    diag_u = guu + ridge
    diag_v = gvv + ridge
    inverse = 1.0 / (diag_u * diag_v - guv * guv)
    base = 1.0 / (count + ridge)
    out = []
    slopes_u, slopes_v = [], []
    for h0, hu, hv in ((h0_re, hu_re, hv_re), (h0_im, hu_im, hv_im)):
        hu = hu - mean_u * h0
        hv = hv - mean_v * h0
        out.append(h0 * base)
        slopes_u.append((diag_v * hu - guv * hv) * inverse)
        slopes_v.append((diag_u * hv - guv * hu) * inverse)
    entries = out + slopes_u + slopes_v + [mean_u, mean_v]
    stacked = jnp.zeros((16, LANES), F32)
    place = row_of((16, LANES))
    for i, entry in enumerate(entries):
        stacked = jnp.where(place == i, entry, stacked)
    stacked = jnp.where(lane_of((16, LANES)) < SWEEP_TALLY, stacked, 0.0)
    high, middle, low = (across_lanes(membership[3], x) for x in split_three(stacked))
    coefs[...] = high + middle + low


def ramp_kernel(count_rows, count_cols, gamma, size, coefs, deramped, coherence, out, sem):
    _, rows, cols = gamma.shape
    my_row = lax.axis_index("rows")
    my_col = lax.axis_index("cols")
    lane = lane_of((8, LANES))
    across_first = ((my_col * cols + lane).astype(F32) + 0.5) * (2.0 / (cols * count_cols)) - 1.0
    chunk = 16
    copies = [pltpu.make_async_copy(size, coherence, sem.at[0])]
    copies[0].start()
    for low in range(0, rows, chunk):
        @pl.loop(low // 8, (low + chunk) // 8)
        def _(group):
            start = pl.multiple_of(group * 8, 8)
            here = pl.ds(start, 8)
            line = coefs[here, :]
            along = ((my_row * rows + start + row_of((8, LANES))).astype(F32) + 0.5) * (
                2.0 / (rows * count_rows)
            ) - 1.0
            wide = [jnp.broadcast_to(line[:, q:q + 1], (8, LANES)) for q in range(8)]
            along = along - wide[7]
            base_re = wide[0] + wide[4] * along
            base_im = wide[1] + wide[5] * along
            centred = across_first - wide[6]
            for j in range(cols // LANES):
                there = pl.ds(j * LANES, LANES)
                du = centred + j * (LANES * 2.0 / (cols * count_cols))
                model_re = base_re + wide[2] * du
                model_im = base_im + wide[3] * du
                real, imag = gamma[0, here, there], gamma[1, here, there]
                out[0, here, there] = real * model_re + imag * model_im
                out[1, here, there] = imag * model_re - real * model_im

        here = pl.ds(low, chunk)
        copy = pltpu.make_async_copy(out.at[:, here, :], deramped.at[:, here, :], sem.at[len(copies)])
        copy.start()
        copies.append(copy)
    for copy in copies:
        copy.wait()


def on_device(count_rows, count_cols, lead, trail, flags, sweep):
    rows, cols = flags.shape
    wide = 2 * LANES
    tiles, between = cols // wide, rows - 2 * HALO
    vmem = pl.BlockSpec(memory_space=pltpu.VMEM)
    hbm = pl.BlockSpec(memory_space=pl.ANY)
    dma = pltpu.SemaphoreType.DMA
    V = pltpu.VMEM
    gamma, size, coefs = pl.pallas_call(
        functools.partial(gamma_kernel, count_rows, count_cols),
        out_shape=(V((2, rows, cols), F32), V((rows, cols), F32), V((rows, 16), F32)),
        in_specs=[hbm, hbm, hbm, hbm],
        out_specs=(vmem, vmem, vmem),
        scratch_shapes=[
            V((2, rows, cols), F32), V((2, rows, cols), F32), V((rows, cols), jnp.int32), V((1, rows), jnp.int32),
            V((4, 2 * rows, cols), BF16),
            V((3, HALO, cols), F32), V((3, HALO, cols), F32), V((3, HALO, cols), F32), V((3, HALO, cols), F32),
            V((2, HALO, LANES), F32), V((2, HALO, LANES), F32),
            V((2, 2, HALO, LANES), F32),
            V((rows, 2 * LANES), F32), V((2 * HALO, 2 * LANES), F32), V((2 * rows, 2 * LANES), BF16), V((4 * HALO, 2 * LANES), BF16),
            V((rows, 2 * rows), BF16), V((2 * HALO, 4 * HALO), BF16),
            V((4, 4 * HALO, cols), BF16), V((wide, wide), BF16), V((wide, wide), BF16),
            V((tiles, 4, between, wide), BF16), V((tiles, 4, between, wide), BF16),
            V((tiles, 4, between, wide), BF16), V((tiles, 4, between, wide), F32),
            V((4, 2 * HALO, cols), F32),
            V((tiles, 4, 2 * HALO, wide), BF16), V((tiles, 4, 2 * HALO, wide), BF16),
            V((tiles, 4, 2 * HALO, wide), BF16), V((tiles, 4, 2 * HALO, wide), F32),
            V((7, between, LANES), F32), V((7, 2 * HALO, LANES), F32),
            V((rows, LANES), F32), V((4, LANES, rows), BF16),
            V((4, LANES), F32), V((3, 4, LANES), F32), V((4, LANES), F32), V((2 * REACH, 4, LANES), F32),
            dma((64,)), dma((2 * PARTS,)), dma((2 * PARTS,)), dma((6,)), dma((6,)), dma((3,)), dma((3,)),
            dma((2 * REACH,)), dma((2 * REACH,)), pltpu.SemaphoreType.REGULAR((5,)),
        ],
        compiler_params=pltpu.CompilerParams(
            collective_id=0, has_side_effects=True, vmem_limit_bytes=63_000_000
        ),
        name="coherence",
    )(lead, trail, flags, sweep.reshape(1, rows))
    return pl.pallas_call(
        functools.partial(ramp_kernel, count_rows, count_cols),
        out_shape=(
            jax.ShapeDtypeStruct((2, rows, cols), F32),
            jax.ShapeDtypeStruct((rows, cols), F32),
        ),
        in_specs=[vmem, vmem, vmem],
        out_specs=(hbm, hbm),
        scratch_shapes=[V((2, rows, cols), F32), dma((9,))],
        compiler_params=pltpu.CompilerParams(vmem_limit_bytes=16 * 1024 * 1024),
        name="ramp",
    )(gamma, size, coefs)


def solution(mesh):
    in_specs = (P(None, "rows", "cols"), P(None, "rows", "cols"), P("rows", "cols"), P("rows"))
    out_specs = (P(None, "rows", "cols"), P("rows", "cols"))
    body = functools.partial(on_device, mesh.shape["rows"], mesh.shape["cols"])
    return jax.shard_map(body, mesh=mesh, in_specs=in_specs, out_specs=out_specs, check_vma=False)
```

```python
import functools

import jax
import jax.numpy as jnp
from jax import lax
from jax.experimental import pallas as pl
from jax.experimental.pallas import tpu as pltpu
from jax.sharding import PartitionSpec as P

WIN_R = 32
WIN_C = 8
SWEEP_TALLY = 16
HALO = WIN_R // 2
SIDE = WIN_C // 2
LANES = 128
REACH = 8
PEERS = 7
PARTS = 4
MESH = pl.DeviceIdType.MESH
F32 = jnp.float32
BF16 = jnp.bfloat16


def split_pair(x):
    high = x.astype(BF16)
    return high, (x - high.astype(F32)).astype(BF16)


def split_three(x):
    high, rest = x.astype(BF16), x - x.astype(BF16).astype(F32)
    return high, rest.astype(BF16), (rest - rest.astype(BF16).astype(F32)).astype(BF16)


def across_lanes(x, y):
    return lax.dot_general(x, y, (((1,), (1,)), ((), ())), preferred_element_type=F32)


def lane_of(shape):
    return lax.broadcasted_iota(jnp.int32, shape, 1)


def row_of(shape):
    return lax.broadcasted_iota(jnp.int32, shape, 0)


def gamma_kernel(
    count_rows, count_cols,
    lead, trail, flags, sweep_in,
    gamma, size, coefs,
    first, second, weight, sweep, planes, up_out, down_out, above, below, side_out, side_in, corner_in,
    side_boxed, side_edge, side_planes, corner_planes, band, tri, halo_planes, across_box, across_join,
    high_in, low_in, join_in, box_in, own_edge, high_edge, low_edge, join_edge, box_edge,
    line_in, line_edge, sums, membership, table, from_cols, table_rows, from_rows,
    load_sem, row_send, row_recv, col_send, col_recv, ysend, yrecv, rsend, rrecv, token,
):
    rows, cols = weight.shape
    blocks = cols // LANES
    my_row = lax.axis_index("rows")
    my_col = lax.axis_index("cols")

    def at(d_row, d_col):
        return {
            "rows": lax.rem(my_row + d_row + count_rows, count_rows),
            "cols": lax.rem(my_col + d_col + count_cols, count_cols),
        }

    def signal(sem, where):
        pl.semaphore_signal(sem, inc=1, device_id=where, device_id_type=MESH)

    barrier = pltpu.get_barrier_semaphore()
    def exists(d_row, d_col=0):
        here, count, d = (my_row, count_rows, d_row) if d_row else (my_col, count_cols, d_col)
        return here >= -d if d < 0 else here < count - d

    def if_there(d_row, d_col, act):
        pl.when(exists(d_row, d_col))(act)

    def tell(sem, distance, along_rows):
        for d in (-distance, distance):
            where = (d, 0) if along_rows else (0, d)
            if_there(*where, lambda where=where: signal(sem, at(*where)))

    def number(distance, along_rows):
        return sum(exists(*((d, 0) if along_rows else (0, d))).astype(jnp.int32) for d in (-distance, distance))

    def hear(sem, distance, along_rows):
        pl.semaphore_wait(sem, number(distance, along_rows))

    tell(barrier, 1, True)
    tell(barrier, 1, False)

    loads = []

    def load(low, high, left, right):
        started = []
        window = (pl.ds(low, high - low), pl.ds(left, right - left))
        for source, target in ((lead, first), (trail, second)):
            started.append((source.at[(slice(None),) + window], target.at[(slice(None),) + window]))
        started.append((flags.at[window], weight.at[window]))
        copies = []
        for source, target in started:
            copy = pltpu.make_async_copy(source, target, load_sem.at[len(loads)])
            copy.start()
            loads.append(copy)
            copies.append(copy)
        return copies

    def arrive(copies):
        for copy in copies:
            copy.wait()

    inner = rows - HALO
    part = cols // PARTS
    edge_loads = []
    sweep_load = pltpu.make_async_copy(sweep_in, sweep, load_sem.at[len(loads)])
    sweep_load.start()
    loads.append(sweep_load)
    for c in range(PARTS):
        right = (c + 1) * part - (LANES if c == PARTS - 1 else 0)
        edge_loads.append(load(0, HALO, c * part, right) + load(inner, rows, c * part, right))
        if c == 0:
            edge_loads[0] += load(0, HALO, cols - LANES, cols) + load(inner, rows, cols - LANES, cols)
    side_loads = load(HALO, inner, 0, LANES) + load(HALO, inner, cols - LANES, cols)
    step = (inner - HALO) // 3
    main_loads = [load(HALO + i * step, HALO + (i + 1) * step, LANES, cols - LANES) for i in range(3)]

    lane = lane_of((8, LANES))
    lane16 = lane_of((HALO, LANES))

    def products(row, block, sends=None):
        here = (pl.ds(row, HALO), pl.ds(block * LANES, LANES))
        w = weight[here].astype(F32)
        real_a, imag_a = first[(0,) + here] * w, first[(1,) + here] * w
        real_b, imag_b = second[(0,) + here], second[(1,) + here]
        power_b = (real_b * real_b + imag_b * imag_b) * w
        if sends is not None:
            real_b, imag_b = real_b * w, imag_b * w
            top = jnp.maximum(jnp.abs(real_b), jnp.abs(imag_b))
            some = top > 0.0
            unit = 1.0 / jnp.where(some, top, 1.0)
            x, y = jnp.where(some, real_b * unit, 1.0), imag_b * unit
            square = x * x + y * y
            turn = lax.rsqrt(square)
            there = here[1]
            sends[0, :, there] = (real_a * x + imag_a * y) * turn
            sends[1, :, there] = (imag_a * x - real_a * y) * turn
            sends[2, :, there] = top * (square * turn)
        return (
            real_a * real_b + imag_a * imag_b,
            imag_a * real_b - real_a * imag_b,
            real_a * real_a + imag_a * imag_a,
            power_b,
        )

    def fill(row, sends=None, some=range(blocks)):
        for block in some:
            here = pl.ds(block * LANES, LANES)
            for p, x in enumerate(products(row, block, sends)):
                high, low = split_pair(x)
                planes[p, pl.ds(row, HALO), here] = high
                planes[p, pl.ds(rows + row, HALO), here] = low

    groups = rows // HALO
    slot = LANES // groups

    def pack(group):
        packed = [jnp.zeros((HALO, LANES), F32) for _ in range(2)]
        for p, x in enumerate(products(group * HALO, 0)):
            x = jnp.where(lane16 < SIDE, x, 0.0)
            packed[0] += x if p == 0 else pltpu.roll(x, SIDE * p, 1)
        for p, x in enumerate(products(group * HALO, blocks - 1)):
            packed[1] += pltpu.roll(jnp.where(lane16 >= LANES - SIDE, x, 0.0), SIDE * (p + 1), 1)
        return packed

    def at_slot(x, group):
        return pltpu.roll(x, slot * group, 1) if group else x

    def send(source, target, send_sem, recv_sem, d_row, d_col, ring=False):
        copy = pltpu.make_async_remote_copy(
            src_ref=source, dst_ref=target, send_sem=send_sem, recv_sem=recv_sem,
            device_id=at(d_row, d_col), device_id_type=MESH,
        )
        if ring:
            copy.start()
        else:
            if_there(d_row, d_col, copy.start)
        return copy, d_row, d_col, ring

    def finish_send(sent):
        copy, d_row, d_col, ring = sent
        if ring:
            copy.wait()
        else:
            if_there(-d_row, -d_col, copy.wait_recv)
            if_there(d_row, d_col, copy.wait_send)

    @pl.when(my_row == 0)
    def _():
        above[...] = jnp.zeros_like(above)
        corner_in[0] = jnp.zeros((2, HALO, LANES), F32)

    @pl.when(my_row == count_rows - 1)
    def _():
        below[...] = jnp.zeros_like(below)
        corner_in[1] = jnp.zeros((2, HALO, LANES), F32)

    for side, missing in enumerate((my_col == 0, my_col == count_cols - 1)):
        @pl.when(missing)
        def _(side=side):
            side_in[side] = jnp.zeros((HALO, LANES), F32)

    distances = [d for k in range(REACH, 0, -2) for d in (-k, k)]
    for i, d in enumerate(distances):
        @pl.when(jnp.logical_not(exists(-d)))
        def _(i=i):
            from_rows[i] = jnp.zeros((4, LANES), F32)

    row_copies = []

    box_row = row_of((rows, 2 * rows))
    box_col = lax.rem(lane_of((rows, 2 * rows)), rows) - box_row
    band[...] = jnp.where((box_col >= -HALO) & (box_col < HALO), 1.0, 0.0).astype(BF16)
    tri_row = row_of((2 * HALO, 4 * HALO))
    tri_lane = lane_of((2 * HALO, 4 * HALO))
    tri_col = lax.rem(tri_lane, HALO)
    has_above = jnp.where(my_row > 0, 1.0, 0.0)
    has_below = jnp.where(my_row < count_rows - 1, 1.0, 0.0)
    tri_above = jnp.where((tri_row < HALO) & (tri_lane < 2 * HALO) & (tri_col >= tri_row), has_above, 0.0)
    tri_below = jnp.where((tri_row >= HALO) & (tri_lane >= 2 * HALO) & (tri_col < tri_row - HALO), has_below, 0.0)
    tri[...] = (tri_above + tri_below).astype(BF16)
    wide = 2 * LANES
    from_lane = row_of((wide, wide))
    to_lane = lane_of((wide, wide))
    apart = from_lane - to_lane
    across_box[...] = jnp.where((apart >= -SIDE) & (apart < SIDE), 1.0, 0.0).astype(BF16)
    from_lane = lax.rem(from_lane, LANES)
    before = (from_lane >= LANES - SIDE) & (to_lane <= from_lane - (LANES - SIDE))
    after = (from_lane < SIDE - 1) & (to_lane >= wide - SIDE + 1 + from_lane)
    across_join[...] = jnp.where(before | after, 1.0, 0.0).astype(BF16)

    def fill_edges(c):
        arrive(edge_loads[c])
        some = range(c * part // LANES, (c + 1) * part // LANES)
        fill(0, up_out, some)
        fill(inner, down_out, some)

    def send_edges(c):
        there = pl.ds(c * part, part)
        row_copies.append([
            send(
                source.at[:, :, there], target.at[:, :, there],
                row_send.at[2 * c + i], row_recv.at[2 * c + i], d_row, 0,
            )
            for i, (source, target, d_row) in enumerate(((up_out, below, -1), (down_out, above, 1)))
        ])

    fill_edges(0)
    pl.semaphore_wait(barrier, number(1, True) + number(1, False))
    send_edges(0)
    fill_edges(1)
    send_edges(1)
    arrive(side_loads)
    lines = [pack(group) for group in range(groups)]
    for side in range(2):
        side_out[side] = sum((at_slot(x[side], group) for group, x in enumerate(lines[1:], 1)), lines[0][side])
    col_copies = [
        send(side_out.at[side], side_in.at[1 - side], col_send.at[side], col_recv.at[side], 0, d_col)
        for side, d_col in enumerate((-1, 1))
    ]
    for c in range(2, PARTS):
        fill_edges(c)
        send_edges(c)
    tell(token.at[0], 1, True)
    tell(token.at[3], 1, False)

    sweep_load.wait()
    along = ((my_row * rows + lane_of((LANES, rows))).astype(F32) + 0.5) * (2.0 / (rows * count_rows)) - 1.0
    burst = row_of((LANES, rows))
    power = burst // SWEEP_TALLY
    chosen = jnp.where((burst - power * SWEEP_TALLY == sweep[...]) & (power < 3), 1.0, 0.0)
    for i, x in enumerate(split_three(chosen * jnp.where(power == 0, 1.0, jnp.where(power == 1, along, along * along)))):
        membership[i] = x
    membership[3] = jnp.transpose(jnp.where(burst == sweep[...], 1.0, 0.0)).astype(BF16)

    for i, copies in enumerate(main_loads):
        arrive(copies)

        @pl.loop(HALO + i * step, HALO + (i + 1) * step, step=HALO)
        def _(row):
            fill(pl.multiple_of(row, HALO))

    tiles = cols // wide
    for n in range(tiles):
        there = pl.ds(n * wide, wide)
        for p in range(4):
            box = jnp.dot(band[...], planes[p, :, there], preferred_element_type=F32)
            high, low = split_pair(box[HALO:inner])
            high_in[n, p] = high
            low_in[n, p] = low
            own_edge[p, pl.ds(0, HALO), there] = box[:HALO]
            own_edge[p, pl.ds(HALO, HALO), there] = box[inner:]

    def join(high_ref, low_ref, join_ref, count, n, packed):
        first_half = lane_of((count, LANES)) < LANES // 2
        parts = [high_ref, low_ref]
        for p in range(4):
            if n == 0:
                outer = split_pair(pltpu.roll(packed[:, :LANES], LANES - SIDE * (p + 1), 1))
            elif n == tiles - 1:
                outer = packed[:, LANES:]
                outer = split_pair(outer if p == 0 else pltpu.roll(outer, LANES - SIDE * p, 1))
            for i in range(2):
                before = outer[i] if n == 0 else parts[i][n - 1, p, :, pl.ds(LANES, LANES)]
                after = outer[i] if n == tiles - 1 else parts[i][n + 1, p, :, pl.ds(0, LANES)]
                join_ref[n, p, :, pl.ds(i * LANES, LANES)] = jnp.where(first_half, after, before)

    def box_across(high_ref, low_ref, join_ref, box_ref, count, n):
        lines = 4 * count
        total = jnp.dot(high_ref[n].reshape(lines, wide), across_box[...], preferred_element_type=F32)
        total += jnp.dot(low_ref[n].reshape(lines, wide), across_box[...], preferred_element_type=F32)
        total += jnp.dot(join_ref[n].reshape(lines, wide), across_join[...], preferred_element_type=F32)
        box_ref[n] = total.reshape(4, count, wide)

    across_first = ((my_col * cols + lane).astype(F32) + 0.5) * (2.0 / (cols * count_cols)) - 1.0

    def finish(box_ref, line_ref, n, at_row, row, fresh):
        here = pl.ds(row, 8)
        totals = None if fresh else [line_ref[q, pl.ds(at_row, 8), :] for q in range(7)]
        for j in (2 * n, 2 * n + 1):
            half = pl.ds(j % 2 * LANES, LANES)
            real, imag, power_a, power_b = (box_ref[n, p, pl.ds(at_row, 8), half] for p in range(4))
            scale = lax.rsqrt((power_a + 1.0) * (power_b + 1.0))
            real, imag = real * scale, imag * scale
            there = pl.ds(j * LANES, LANES)
            gamma[0, here, there] = real
            gamma[1, here, there] = imag
            w = weight[here, there].astype(F32)
            across = across_first + j * (LANES * 2.0 / (cols * count_cols))
            wu = w * across
            terms = (w, wu, wu * across, w * real, w * imag, wu * real, wu * imag)
            totals = list(terms) if totals is None else [total + term for total, term in zip(totals, terms)]
        for q, total in enumerate(totals):
            line_ref[q, pl.ds(at_row, 8), :] = total

    def gather_lines(line_ref, at_row, row):
        line = jnp.zeros((8, LANES), F32)
        for q in range(7):
            line = jnp.where(lane == q, jnp.sum(line_ref[q, pl.ds(at_row, 8), :], axis=1, keepdims=True), line)
        sums[pl.ds(row, 8), :] = line

    between = inner - HALO

    def run_inner(order, fresh_at, packed=None):
        waiting = None
        for n in order + [None]:
            if n is not None:
                join(high_in, low_in, join_in, between, n, packed)
                box_across(high_in, low_in, join_in, box_in, between, n)
            if waiting is not None:
                for at_row in range(0, between, 8):
                    finish(box_in, line_in, waiting, at_row, at_row + HALO, waiting == fresh_at)
            waiting = n

    for sent in col_copies:
        finish_send(sent)
    corner_copies = [
        send(side_in, corner_in.at[1 - k], col_send.at[2 + k], col_recv.at[2 + k], d_row, 0)
        for k, d_row in enumerate((-1, 1))
    ]
    run_inner(list(range(1, tiles - 1)), 1)

    hear(token.at[0], 1, True)
    tell(token.at[1], 2, True)
    hear(token.at[3], 1, False)
    tell(token.at[4], 2, False)

    side_exists = [jnp.where(my_col > 0, 1.0, 0.0), jnp.where(my_col < count_cols - 1, 1.0, 0.0)]
    for i in range(2):
        there = pl.ds(i * LANES, LANES)
        arrived = side_in[i] * side_exists[i]
        for group in range(groups):
            high, low = split_pair(pltpu.roll(arrived, LANES - slot * group, 1) if group else arrived)
            side_planes[pl.ds(group * HALO, HALO), there] = high
            side_planes[pl.ds(rows + group * HALO, HALO), there] = low
    side_boxed[...] = jnp.dot(band[...], side_planes[...], preferred_element_type=F32)
    run_inner([0, tiles - 1], None, side_boxed[pl.ds(HALO, between), :])
    for at_row in range(0, between, 8):
        gather_lines(line_in, at_row, at_row + HALO)

    for group in ((0, 1), (2,), (3,)):
        for c in group:
            for sent in row_copies[c]:
                finish_send(sent)
        start, last = group[0] * part // wide, (group[-1] + 1) * part // wide
        here = pl.ds(start * wide, (last - start) * wide)
        for i, arrived in enumerate((above, below)):
            turned_re, turned_im, length = (arrived[q, :, here] for q in range(3))
            arrived_planes = (
                turned_re * length, turned_im * length, turned_re * turned_re + turned_im * turned_im, length * length
            )
            for p, x in enumerate(arrived_planes):
                high, low = split_pair(x)
                halo_planes[p, pl.ds(2 * i * HALO, HALO), here] = high
                halo_planes[p, pl.ds((2 * i + 1) * HALO, HALO), here] = low
        for n in range(start, last):
            there = pl.ds(n * wide, wide)
            for p in range(4):
                extra = jnp.dot(tri[...], halo_planes[p, :, there], preferred_element_type=F32)
                high, low = split_pair(own_edge[p, :, there] + extra)
                high_edge[n, p] = high
                low_edge[n, p] = low
        if last == tiles:
            for sent in corner_copies:
                finish_send(sent)
            for i in range(2):
                there = pl.ds(i * LANES, LANES)
                for k in range(2):
                    arrived = corner_in[k, i] * side_exists[i]
                    high, low = split_pair(arrived if k else pltpu.roll(arrived, slot, 1))
                    corner_planes[pl.ds(2 * k * HALO, HALO), there] = high
                    corner_planes[pl.ds((2 * k + 1) * HALO, HALO), there] = low
            side_edge[...] = jnp.dot(tri[...], corner_planes[...], preferred_element_type=F32) + jnp.concatenate(
                [side_boxed[pl.ds(0, HALO), :], side_boxed[pl.ds(inner, HALO), :]], axis=0
            )
        ends_at = list(range(max(start - 1, 1), last - 1)) + ([tiles - 1, 0] if last == tiles else [])
        for n in ends_at:
            join(high_edge, low_edge, join_edge, 2 * HALO, n, side_edge[...] if last == tiles else None)
            box_across(high_edge, low_edge, join_edge, box_edge, 2 * HALO, n)
        for n in ends_at:
            for at_row in range(0, 2 * HALO, 8):
                finish(box_edge, line_edge, n, at_row, at_row if at_row < HALO else at_row - HALO + inner, n == 1)
    for at_row in range(0, 2 * HALO, 8):
        gather_lines(line_edge, at_row, at_row if at_row < HALO else at_row - HALO + inner)

    lines = split_three(jnp.transpose(sums[...])[:16])
    full = sum(across_lanes(lines[i], membership[j]) for i, j in ((2, 0), (0, 2), (1, 1), (1, 0), (0, 1), (0, 0)))[:8]
    table[...] = full[:4] + pltpu.roll(full[4:], LANES // 2, 1)

    hear(token.at[4], 2, False)
    partner = 1 - 2 * lax.rem(my_row, 2)
    copies = [
        send(table, from_cols.at[i], ysend.at[i], yrecv.at[i], partner if other else 0, k, True)
        for i, (other, k) in enumerate(((1, 2), (0, 2), (1, 1), (1, 3), (0, 1), (0, 3), (1, 0)))
    ]
    hear(token.at[1], 2, True)
    tell(token.at[2], 4, True)
    hear(token.at[2], 4, True)
    for sent in copies:
        finish_send(sent)
    table_rows[...] = sum((from_cols[i] for i in range(PEERS)), table[...])
    copies = [
        send(table_rows, from_rows.at[i], rsend.at[i], rrecv.at[i], d, 0) for i, d in enumerate(distances)
    ]

    @pl.loop(0, rows // 8)
    def _(group):
        here = pl.ds(pl.multiple_of(group * 8, 8), 8)
        for j in range(blocks):
            there = pl.ds(j * LANES, LANES)
            real, imag = gamma[0, here, there], gamma[1, here, there]
            size[here, there] = jnp.sqrt(real * real + imag * imag)

    for sent in copies:
        finish_send(sent)
    total = table_rows[...]
    for i in range(len(distances)):
        total = total + from_rows[i]

    total = jnp.concatenate([total, pltpu.roll(total, LANES // 2, 1)], axis=0)
    once = pltpu.roll(total, LANES - SWEEP_TALLY, 1)
    twice = pltpu.roll(total, LANES - 2 * SWEEP_TALLY, 1)
    count, sum_u, sum_uu, h0_re, h0_im, hu_re, hu_im = (total[q:q + 1] for q in range(7))
    sum_v, sum_uv, hv_re, hv_im = (once[q:q + 1] for q in (0, 1, 3, 4))
    sum_vv = twice[0:1]
    floored = jnp.maximum(count, 1.0)
    mean_u = sum_u / floored
    mean_v = sum_v / floored
    guu = sum_uu - 2.0 * mean_u * sum_u + mean_u * mean_u * count
    guv = sum_uv - mean_u * sum_v - mean_v * sum_u + mean_u * mean_v * count
    gvv = sum_vv - 2.0 * mean_v * sum_v + mean_v * mean_v * count
    ridge = 0.001 * count + 1.0
    diag_u = guu + ridge
    diag_v = gvv + ridge
    inverse = 1.0 / (diag_u * diag_v - guv * guv)
    base = 1.0 / (count + ridge)
    out = []
    slopes_u, slopes_v = [], []
    for h0, hu, hv in ((h0_re, hu_re, hv_re), (h0_im, hu_im, hv_im)):
        hu = hu - mean_u * h0
        hv = hv - mean_v * h0
        out.append(h0 * base)
        slopes_u.append((diag_v * hu - guv * hv) * inverse)
        slopes_v.append((diag_u * hv - guv * hu) * inverse)
    entries = out + slopes_u + slopes_v + [mean_u, mean_v]
    stacked = jnp.zeros((16, LANES), F32)
    place = row_of((16, LANES))
    for i, entry in enumerate(entries):
        stacked = jnp.where(place == i, entry, stacked)
    stacked = jnp.where(lane_of((16, LANES)) < SWEEP_TALLY, stacked, 0.0)
    high, middle, low = (across_lanes(membership[3], x) for x in split_three(stacked))
    coefs[...] = high + middle + low


def ramp_kernel(count_rows, count_cols, gamma, size, coefs, deramped, coherence, out, sem):
    _, rows, cols = gamma.shape
    my_row = lax.axis_index("rows")
    my_col = lax.axis_index("cols")
    lane = lane_of((8, LANES))
    across_first = ((my_col * cols + lane).astype(F32) + 0.5) * (2.0 / (cols * count_cols)) - 1.0
    chunk = 16
    copies = [pltpu.make_async_copy(size, coherence, sem.at[0])]
    copies[0].start()
    for low in range(0, rows, chunk):
        @pl.loop(low // 8, (low + chunk) // 8)
        def _(group):
            start = pl.multiple_of(group * 8, 8)
            here = pl.ds(start, 8)
            line = coefs[here, :]
            along = ((my_row * rows + start + row_of((8, LANES))).astype(F32) + 0.5) * (
                2.0 / (rows * count_rows)
            ) - 1.0
            wide = [jnp.broadcast_to(line[:, q:q + 1], (8, LANES)) for q in range(8)]
            along = along - wide[7]
            base_re = wide[0] + wide[4] * along
            base_im = wide[1] + wide[5] * along
            centred = across_first - wide[6]
            for j in range(cols // LANES):
                there = pl.ds(j * LANES, LANES)
                du = centred + j * (LANES * 2.0 / (cols * count_cols))
                model_re = base_re + wide[2] * du
                model_im = base_im + wide[3] * du
                real, imag = gamma[0, here, there], gamma[1, here, there]
                out[0, here, there] = real * model_re + imag * model_im
                out[1, here, there] = imag * model_re - real * model_im

        here = pl.ds(low, chunk)
        copy = pltpu.make_async_copy(out.at[:, here, :], deramped.at[:, here, :], sem.at[len(copies)])
        copy.start()
        copies.append(copy)
    for copy in copies:
        copy.wait()


def on_device(count_rows, count_cols, lead, trail, flags, sweep):
    rows, cols = flags.shape
    wide = 2 * LANES
    tiles, between = cols // wide, rows - 2 * HALO
    vmem = pl.BlockSpec(memory_space=pltpu.VMEM)
    hbm = pl.BlockSpec(memory_space=pl.ANY)
    dma = pltpu.SemaphoreType.DMA
    V = pltpu.VMEM
    gamma, size, coefs = pl.pallas_call(
        functools.partial(gamma_kernel, count_rows, count_cols),
        out_shape=(V((2, rows, cols), F32), V((rows, cols), F32), V((rows, 16), F32)),
        in_specs=[hbm, hbm, hbm, hbm],
        out_specs=(vmem, vmem, vmem),
        scratch_shapes=[
            V((2, rows, cols), F32), V((2, rows, cols), F32), V((rows, cols), jnp.int32), V((1, rows), jnp.int32),
            V((4, 2 * rows, cols), BF16),
            V((3, HALO, cols), F32), V((3, HALO, cols), F32), V((3, HALO, cols), F32), V((3, HALO, cols), F32),
            V((2, HALO, LANES), F32), V((2, HALO, LANES), F32),
            V((2, 2, HALO, LANES), F32),
            V((rows, 2 * LANES), F32), V((2 * HALO, 2 * LANES), F32), V((2 * rows, 2 * LANES), BF16), V((4 * HALO, 2 * LANES), BF16),
            V((rows, 2 * rows), BF16), V((2 * HALO, 4 * HALO), BF16),
            V((4, 4 * HALO, cols), BF16), V((wide, wide), BF16), V((wide, wide), BF16),
            V((tiles, 4, between, wide), BF16), V((tiles, 4, between, wide), BF16),
            V((tiles, 4, between, wide), BF16), V((tiles, 4, between, wide), F32),
            V((4, 2 * HALO, cols), F32),
            V((tiles, 4, 2 * HALO, wide), BF16), V((tiles, 4, 2 * HALO, wide), BF16),
            V((tiles, 4, 2 * HALO, wide), BF16), V((tiles, 4, 2 * HALO, wide), F32),
            V((7, between, LANES), F32), V((7, 2 * HALO, LANES), F32),
            V((rows, LANES), F32), V((4, LANES, rows), BF16),
            V((4, LANES), F32), V((PEERS, 4, LANES), F32), V((4, LANES), F32), V((REACH, 4, LANES), F32),
            dma((64,)), dma((2 * PARTS,)), dma((2 * PARTS,)), dma((4,)), dma((4,)), dma((PEERS,)), dma((PEERS,)),
            dma((REACH,)), dma((REACH,)), pltpu.SemaphoreType.REGULAR((5,)),
        ],
        compiler_params=pltpu.CompilerParams(
            collective_id=0, has_side_effects=True, vmem_limit_bytes=63_000_000
        ),
        name="coherence",
    )(lead, trail, flags, sweep.reshape(1, rows))
    return pl.pallas_call(
        functools.partial(ramp_kernel, count_rows, count_cols),
        out_shape=(
            jax.ShapeDtypeStruct((2, rows, cols), F32),
            jax.ShapeDtypeStruct((rows, cols), F32),
        ),
        in_specs=[vmem, vmem, vmem],
        out_specs=(hbm, hbm),
        scratch_shapes=[V((2, rows, cols), F32), dma((9,))],
        compiler_params=pltpu.CompilerParams(vmem_limit_bytes=16 * 1024 * 1024),
        name="ramp",
    )(gamma, size, coefs)


def solution(mesh):
    in_specs = (P(None, "rows", "cols"), P(None, "rows", "cols"), P("rows", "cols"), P("rows"))
    out_specs = (P(None, "rows", "cols"), P("rows", "cols"))
    body = functools.partial(on_device, mesh.shape["rows"], mesh.shape["cols"])
    return jax.shard_map(body, mesh=mesh, in_specs=in_specs, out_specs=out_specs, check_vma=False)
```

```python
import functools

import jax
import jax.numpy as jnp
from jax import lax
from jax.experimental import pallas as pl
from jax.experimental.pallas import tpu as pltpu
from jax.sharding import PartitionSpec as P

WIN_R = 32
WIN_C = 8
SWEEP_TALLY = 16
HALO = WIN_R // 2
SIDE = WIN_C // 2
LANES = 128
REACH = 8
PEERS = 7
PARTS = 4
TINY = 1.1754944e-38
MESH = pl.DeviceIdType.MESH
F32 = jnp.float32
BF16 = jnp.bfloat16


def split_pair(x):
    high = x.astype(BF16)
    return high, (x - high.astype(F32)).astype(BF16)


def split_three(x):
    high, rest = x.astype(BF16), x - x.astype(BF16).astype(F32)
    return high, rest.astype(BF16), (rest - rest.astype(BF16).astype(F32)).astype(BF16)


def across_lanes(x, y):
    return lax.dot_general(x, y, (((1,), (1,)), ((), ())), preferred_element_type=F32)


def lane_of(shape):
    return lax.broadcasted_iota(jnp.int32, shape, 1)


def row_of(shape):
    return lax.broadcasted_iota(jnp.int32, shape, 0)


def gamma_kernel(
    count_rows, count_cols,
    lead, trail, flags, sweep_in,
    gamma, size, coefs,
    first, second, weight, sweep, planes, up_out, down_out, above, below, side_out, side_in, corner_in,
    side_boxed, side_edge, side_planes, corner_planes, band, tri, halo_planes, across_box, across_join,
    high_in, low_in, join_in, box_in, own_edge, high_edge, low_edge, join_edge, box_edge,
    line_in, line_edge, sums, membership, table, from_cols, table_rows, from_rows,
    load_sem, row_send, row_recv, col_send, col_recv, ysend, yrecv, rsend, rrecv, token,
):
    rows, cols = weight.shape
    blocks = cols // LANES
    my_row = lax.axis_index("rows")
    my_col = lax.axis_index("cols")

    def at(d_row, d_col):
        return {
            "rows": lax.rem(my_row + d_row + count_rows, count_rows),
            "cols": lax.rem(my_col + d_col + count_cols, count_cols),
        }

    def signal(sem, where):
        pl.semaphore_signal(sem, inc=1, device_id=where, device_id_type=MESH)

    barrier = pltpu.get_barrier_semaphore()
    def exists(d_row, d_col=0):
        here, count, d = (my_row, count_rows, d_row) if d_row else (my_col, count_cols, d_col)
        return here >= -d if d < 0 else here < count - d

    def if_there(d_row, d_col, act):
        pl.when(exists(d_row, d_col))(act)

    def tell(sem, distance, along_rows):
        for d in (-distance, distance):
            where = (d, 0) if along_rows else (0, d)
            if_there(*where, lambda where=where: signal(sem, at(*where)))

    def number(distance, along_rows):
        return sum(exists(*((d, 0) if along_rows else (0, d))).astype(jnp.int32) for d in (-distance, distance))

    def hear(sem, distance, along_rows):
        pl.semaphore_wait(sem, number(distance, along_rows))

    tell(barrier, 1, True)
    tell(barrier, 1, False)

    loads = []

    def load(low, high, left, right):
        started = []
        window = (pl.ds(low, high - low), pl.ds(left, right - left))
        for source, target in ((lead, first), (trail, second)):
            started.append((source.at[(slice(None),) + window], target.at[(slice(None),) + window]))
        started.append((flags.at[window], weight.at[window]))
        copies = []
        for source, target in started:
            copy = pltpu.make_async_copy(source, target, load_sem.at[len(loads)])
            copy.start()
            loads.append(copy)
            copies.append(copy)
        return copies

    def arrive(copies):
        for copy in copies:
            copy.wait()

    inner = rows - HALO
    part = cols // PARTS
    edge_loads = []
    sweep_load = pltpu.make_async_copy(sweep_in, sweep, load_sem.at[len(loads)])
    sweep_load.start()
    loads.append(sweep_load)
    for c in range(PARTS):
        right = (c + 1) * part - (LANES if c == PARTS - 1 else 0)
        edge_loads.append(load(0, HALO, c * part, right) + load(inner, rows, c * part, right))
        if c == 0:
            edge_loads[0] += load(0, HALO, cols - LANES, cols) + load(inner, rows, cols - LANES, cols)
    side_loads = load(HALO, inner, 0, LANES) + load(HALO, inner, cols - LANES, cols)
    step = (inner - HALO) // 3
    main_loads = [load(HALO + i * step, HALO + (i + 1) * step, LANES, cols - LANES) for i in range(3)]

    lane = lane_of((8, LANES))
    lane16 = lane_of((HALO, LANES))

    def products(row, block, sends=None):
        here = (pl.ds(row, HALO), pl.ds(block * LANES, LANES))
        w = weight[here].astype(F32)
        real_a, imag_a = first[(0,) + here] * w, first[(1,) + here] * w
        real_b, imag_b = second[(0,) + here], second[(1,) + here]
        power_b = (real_b * real_b + imag_b * imag_b) * w
        if sends is not None:
            real_b, imag_b = real_b * w, imag_b * w
            top = jnp.maximum(jnp.abs(real_b), jnp.abs(imag_b))
            some = top >= TINY
            unit = 1.0 / jnp.where(some, top, 1.0)
            x, y = jnp.where(some, real_b * unit, 1.0), imag_b * unit
            square = x * x + y * y
            turn = lax.rsqrt(square)
            there = here[1]
            sends[0, :, there] = (real_a * x + imag_a * y) * turn
            sends[1, :, there] = (imag_a * x - real_a * y) * turn
            sends[2, :, there] = top * (square * turn)
        return (
            real_a * real_b + imag_a * imag_b,
            imag_a * real_b - real_a * imag_b,
            real_a * real_a + imag_a * imag_a,
            power_b,
        )

    def fill(row, sends=None, some=range(blocks)):
        for block in some:
            here = pl.ds(block * LANES, LANES)
            for p, x in enumerate(products(row, block, sends)):
                high, low = split_pair(x)
                planes[p, pl.ds(row, HALO), here] = high
                planes[p, pl.ds(rows + row, HALO), here] = low

    groups = rows // HALO
    slot = LANES // groups

    def pack(group):
        packed = [jnp.zeros((HALO, LANES), F32) for _ in range(2)]
        for p, x in enumerate(products(group * HALO, 0)):
            x = jnp.where(lane16 < SIDE, x, 0.0)
            packed[0] += x if p == 0 else pltpu.roll(x, SIDE * p, 1)
        for p, x in enumerate(products(group * HALO, blocks - 1)):
            packed[1] += pltpu.roll(jnp.where(lane16 >= LANES - SIDE, x, 0.0), SIDE * (p + 1), 1)
        return packed

    def at_slot(x, group):
        return pltpu.roll(x, slot * group, 1) if group else x

    def send(source, target, send_sem, recv_sem, d_row, d_col, ring=False):
        copy = pltpu.make_async_remote_copy(
            src_ref=source, dst_ref=target, send_sem=send_sem, recv_sem=recv_sem,
            device_id=at(d_row, d_col), device_id_type=MESH,
        )
        if ring:
            copy.start()
        else:
            if_there(d_row, d_col, copy.start)
        return copy, d_row, d_col, ring

    def finish_send(sent):
        copy, d_row, d_col, ring = sent
        if ring:
            copy.wait()
        else:
            if_there(-d_row, -d_col, copy.wait_recv)
            if_there(d_row, d_col, copy.wait_send)

    @pl.when(my_row == 0)
    def _():
        above[...] = jnp.zeros_like(above)
        corner_in[0] = jnp.zeros((2, HALO, LANES), F32)

    @pl.when(my_row == count_rows - 1)
    def _():
        below[...] = jnp.zeros_like(below)
        corner_in[1] = jnp.zeros((2, HALO, LANES), F32)

    for side, missing in enumerate((my_col == 0, my_col == count_cols - 1)):
        @pl.when(missing)
        def _(side=side):
            side_in[side] = jnp.zeros((HALO, LANES), F32)

    distances = [d for k in range(REACH, 0, -2) for d in (-k, k)]
    for i, d in enumerate(distances):
        @pl.when(jnp.logical_not(exists(-d)))
        def _(i=i):
            from_rows[i] = jnp.zeros((4, LANES), F32)

    row_copies = []

    box_row = row_of((rows, 2 * rows))
    box_col = lax.rem(lane_of((rows, 2 * rows)), rows) - box_row
    band[...] = jnp.where((box_col >= -HALO) & (box_col < HALO), 1.0, 0.0).astype(BF16)
    tri_row = row_of((2 * HALO, 4 * HALO))
    tri_lane = lane_of((2 * HALO, 4 * HALO))
    tri_col = lax.rem(tri_lane, HALO)
    has_above = jnp.where(my_row > 0, 1.0, 0.0)
    has_below = jnp.where(my_row < count_rows - 1, 1.0, 0.0)
    tri_above = jnp.where((tri_row < HALO) & (tri_lane < 2 * HALO) & (tri_col >= tri_row), has_above, 0.0)
    tri_below = jnp.where((tri_row >= HALO) & (tri_lane >= 2 * HALO) & (tri_col < tri_row - HALO), has_below, 0.0)
    tri[...] = (tri_above + tri_below).astype(BF16)
    wide = 2 * LANES
    from_lane = row_of((wide, wide))
    to_lane = lane_of((wide, wide))
    apart = from_lane - to_lane
    across_box[...] = jnp.where((apart >= -SIDE) & (apart < SIDE), 1.0, 0.0).astype(BF16)
    from_lane = lax.rem(from_lane, LANES)
    before = (from_lane >= LANES - SIDE) & (to_lane <= from_lane - (LANES - SIDE))
    after = (from_lane < SIDE - 1) & (to_lane >= wide - SIDE + 1 + from_lane)
    across_join[...] = jnp.where(before | after, 1.0, 0.0).astype(BF16)

    def fill_edges(c):
        arrive(edge_loads[c])
        some = range(c * part // LANES, (c + 1) * part // LANES)
        fill(0, up_out, some)
        fill(inner, down_out, some)

    def send_edges(c):
        there = pl.ds(c * part, part)
        row_copies.append([
            send(
                source.at[:, :, there], target.at[:, :, there],
                row_send.at[2 * c + i], row_recv.at[2 * c + i], d_row, 0,
            )
            for i, (source, target, d_row) in enumerate(((up_out, below, -1), (down_out, above, 1)))
        ])

    fill_edges(0)
    sweep_load.wait()
    along = ((my_row * rows + lane_of((LANES, rows))).astype(F32) + 0.5) * (2.0 / (rows * count_rows)) - 1.0
    burst = row_of((LANES, rows))
    power = burst // SWEEP_TALLY
    chosen = jnp.where((burst - power * SWEEP_TALLY == sweep[...]) & (power < 3), 1.0, 0.0)
    for i, x in enumerate(split_three(chosen * jnp.where(power == 0, 1.0, jnp.where(power == 1, along, along * along)))):
        membership[i] = x
    membership[3] = jnp.transpose(jnp.where(burst == sweep[...], 1.0, 0.0)).astype(BF16)
    pl.semaphore_wait(barrier, number(1, True) + number(1, False))
    send_edges(0)
    fill_edges(1)
    send_edges(1)
    arrive(side_loads)
    lines = [pack(group) for group in range(groups)]
    for side in range(2):
        side_out[side] = sum((at_slot(x[side], group) for group, x in enumerate(lines[1:], 1)), lines[0][side])
    col_copies = [
        send(side_out.at[side], side_in.at[1 - side], col_send.at[side], col_recv.at[side], 0, d_col)
        for side, d_col in enumerate((-1, 1))
    ]
    for c in range(2, PARTS):
        fill_edges(c)
        send_edges(c)
    tell(token.at[0], 1, True)
    tell(token.at[3], 1, False)

    for i, copies in enumerate(main_loads):
        arrive(copies)

        @pl.loop(HALO + i * step, HALO + (i + 1) * step, step=HALO)
        def _(row):
            fill(pl.multiple_of(row, HALO))

    tiles = cols // wide
    for n in range(tiles):
        there = pl.ds(n * wide, wide)
        for p in range(4):
            box = jnp.dot(band[...], planes[p, :, there], preferred_element_type=F32)
            high, low = split_pair(box[HALO:inner])
            high_in[n, p] = high
            low_in[n, p] = low
            own_edge[p, pl.ds(0, HALO), there] = box[:HALO]
            own_edge[p, pl.ds(HALO, HALO), there] = box[inner:]

    def join(high_ref, low_ref, join_ref, count, n, packed):
        first_half = lane_of((count, LANES)) < LANES // 2
        parts = [high_ref, low_ref]
        for p in range(4):
            if n == 0:
                outer = split_pair(pltpu.roll(packed[:, :LANES], LANES - SIDE * (p + 1), 1))
            elif n == tiles - 1:
                outer = packed[:, LANES:]
                outer = split_pair(outer if p == 0 else pltpu.roll(outer, LANES - SIDE * p, 1))
            for i in range(2):
                before = outer[i] if n == 0 else parts[i][n - 1, p, :, pl.ds(LANES, LANES)]
                after = outer[i] if n == tiles - 1 else parts[i][n + 1, p, :, pl.ds(0, LANES)]
                join_ref[n, p, :, pl.ds(i * LANES, LANES)] = jnp.where(first_half, after, before)

    def box_across(high_ref, low_ref, join_ref, box_ref, count, n):
        lines = 4 * count
        total = jnp.dot(high_ref[n].reshape(lines, wide), across_box[...], preferred_element_type=F32)
        total += jnp.dot(low_ref[n].reshape(lines, wide), across_box[...], preferred_element_type=F32)
        total += jnp.dot(join_ref[n].reshape(lines, wide), across_join[...], preferred_element_type=F32)
        box_ref[n] = total.reshape(4, count, wide)

    across_first = ((my_col * cols + lane).astype(F32) + 0.5) * (2.0 / (cols * count_cols)) - 1.0

    def finish(box_ref, line_ref, n, at_row, row, fresh):
        here = pl.ds(row, 8)
        totals = None if fresh else [line_ref[q, pl.ds(at_row, 8), :] for q in range(7)]
        for j in (2 * n, 2 * n + 1):
            half = pl.ds(j % 2 * LANES, LANES)
            real, imag, power_a, power_b = (box_ref[n, p, pl.ds(at_row, 8), half] for p in range(4))
            scale = lax.rsqrt((power_a + 1.0) * (power_b + 1.0))
            real, imag = real * scale, imag * scale
            there = pl.ds(j * LANES, LANES)
            gamma[0, here, there] = real
            gamma[1, here, there] = imag
            w = weight[here, there].astype(F32)
            across = across_first + j * (LANES * 2.0 / (cols * count_cols))
            wu = w * across
            terms = (w, wu, wu * across, w * real, w * imag, wu * real, wu * imag)
            totals = list(terms) if totals is None else [total + term for total, term in zip(totals, terms)]
        for q, total in enumerate(totals):
            line_ref[q, pl.ds(at_row, 8), :] = total

    def gather_lines(line_ref, at_row, row):
        line = jnp.zeros((8, LANES), F32)
        for q in range(7):
            line = jnp.where(lane == q, jnp.sum(line_ref[q, pl.ds(at_row, 8), :], axis=1, keepdims=True), line)
        sums[pl.ds(row, 8), :] = line

    between = inner - HALO

    def run_inner(order, fresh_at, packed=None):
        waiting = None
        for n in order + [None]:
            if n is not None:
                join(high_in, low_in, join_in, between, n, packed)
                box_across(high_in, low_in, join_in, box_in, between, n)
            if waiting is not None:
                for at_row in range(0, between, 8):
                    finish(box_in, line_in, waiting, at_row, at_row + HALO, waiting == fresh_at)
            waiting = n

    for sent in col_copies:
        finish_send(sent)
    corner_copies = [
        send(side_in, corner_in.at[1 - k], col_send.at[2 + k], col_recv.at[2 + k], d_row, 0)
        for k, d_row in enumerate((-1, 1))
    ]
    run_inner(list(range(1, tiles - 1)), 1)

    hear(token.at[0], 1, True)
    tell(token.at[1], 2, True)
    hear(token.at[3], 1, False)
    tell(token.at[4], 2, False)

    side_exists = [jnp.where(my_col > 0, 1.0, 0.0), jnp.where(my_col < count_cols - 1, 1.0, 0.0)]
    for i in range(2):
        there = pl.ds(i * LANES, LANES)
        arrived = side_in[i] * side_exists[i]
        for group in range(groups):
            high, low = split_pair(pltpu.roll(arrived, LANES - slot * group, 1) if group else arrived)
            side_planes[pl.ds(group * HALO, HALO), there] = high
            side_planes[pl.ds(rows + group * HALO, HALO), there] = low
    side_boxed[...] = jnp.dot(band[...], side_planes[...], preferred_element_type=F32)
    run_inner([0, tiles - 1], None, side_boxed[pl.ds(HALO, between), :])
    for at_row in range(0, between, 8):
        gather_lines(line_in, at_row, at_row + HALO)

    for group in ((0, 1), (2,), (3,)):
        for c in group:
            for sent in row_copies[c]:
                finish_send(sent)
        start, last = group[0] * part // wide, (group[-1] + 1) * part // wide
        here = pl.ds(start * wide, (last - start) * wide)
        for i, arrived in enumerate((above, below)):
            turned_re, turned_im, length = (arrived[q, :, here] for q in range(3))
            arrived_planes = (
                turned_re * length, turned_im * length, turned_re * turned_re + turned_im * turned_im, length * length
            )
            for p, x in enumerate(arrived_planes):
                high, low = split_pair(x)
                halo_planes[p, pl.ds(2 * i * HALO, HALO), here] = high
                halo_planes[p, pl.ds((2 * i + 1) * HALO, HALO), here] = low
        for n in range(start, last):
            there = pl.ds(n * wide, wide)
            for p in range(4):
                extra = jnp.dot(tri[...], halo_planes[p, :, there], preferred_element_type=F32)
                high, low = split_pair(own_edge[p, :, there] + extra)
                high_edge[n, p] = high
                low_edge[n, p] = low
        if last == tiles:
            for sent in corner_copies:
                finish_send(sent)
            for i in range(2):
                there = pl.ds(i * LANES, LANES)
                for k in range(2):
                    arrived = corner_in[k, i] * side_exists[i]
                    high, low = split_pair(arrived if k else pltpu.roll(arrived, slot, 1))
                    corner_planes[pl.ds(2 * k * HALO, HALO), there] = high
                    corner_planes[pl.ds((2 * k + 1) * HALO, HALO), there] = low
            side_edge[...] = jnp.dot(tri[...], corner_planes[...], preferred_element_type=F32) + jnp.concatenate(
                [side_boxed[pl.ds(0, HALO), :], side_boxed[pl.ds(inner, HALO), :]], axis=0
            )
        ends_at = list(range(max(start - 1, 1), last - 1)) + ([tiles - 1, 0] if last == tiles else [])
        for n in ends_at:
            join(high_edge, low_edge, join_edge, 2 * HALO, n, side_edge[...] if last == tiles else None)
            box_across(high_edge, low_edge, join_edge, box_edge, 2 * HALO, n)
        for n in ends_at:
            for at_row in range(0, 2 * HALO, 8):
                finish(box_edge, line_edge, n, at_row, at_row if at_row < HALO else at_row - HALO + inner, n == 1)
    for at_row in range(0, 2 * HALO, 8):
        gather_lines(line_edge, at_row, at_row if at_row < HALO else at_row - HALO + inner)

    lines = split_three(jnp.transpose(sums[...])[:16])
    full = sum(across_lanes(lines[i], membership[j]) for i, j in ((2, 0), (0, 2), (1, 1), (1, 0), (0, 1), (0, 0)))[:8]
    table[...] = full[:4] + pltpu.roll(full[4:], LANES // 2, 1)

    hear(token.at[4], 2, False)
    partner = 1 - 2 * lax.rem(my_row, 2)
    copies = [
        send(table, from_cols.at[i], ysend.at[i], yrecv.at[i], partner if other else 0, k, True)
        for i, (other, k) in enumerate(((1, 2), (0, 2), (1, 1), (1, 3), (0, 1), (0, 3), (1, 0)))
    ]
    hear(token.at[1], 2, True)
    tell(token.at[2], 4, True)
    hear(token.at[2], 4, True)
    for sent in copies:
        finish_send(sent)
    table_rows[...] = sum((from_cols[i] for i in range(PEERS)), table[...])
    copies = [
        send(table_rows, from_rows.at[i], rsend.at[i], rrecv.at[i], d, 0) for i, d in enumerate(distances)
    ]

    @pl.loop(0, rows // 8)
    def _(group):
        here = pl.ds(pl.multiple_of(group * 8, 8), 8)
        for j in range(blocks):
            there = pl.ds(j * LANES, LANES)
            real, imag = gamma[0, here, there], gamma[1, here, there]
            size[here, there] = jnp.sqrt(real * real + imag * imag)

    for sent in copies:
        finish_send(sent)
    total = table_rows[...]
    for i in range(len(distances)):
        total = total + from_rows[i]

    total = jnp.concatenate([total, pltpu.roll(total, LANES // 2, 1)], axis=0)
    once = pltpu.roll(total, LANES - SWEEP_TALLY, 1)
    twice = pltpu.roll(total, LANES - 2 * SWEEP_TALLY, 1)
    count, sum_u, sum_uu, h0_re, h0_im, hu_re, hu_im = (total[q:q + 1] for q in range(7))
    sum_v, sum_uv, hv_re, hv_im = (once[q:q + 1] for q in (0, 1, 3, 4))
    sum_vv = twice[0:1]
    floored = jnp.maximum(count, 1.0)
    mean_u = sum_u / floored
    mean_v = sum_v / floored
    guu = sum_uu - 2.0 * mean_u * sum_u + mean_u * mean_u * count
    guv = sum_uv - mean_u * sum_v - mean_v * sum_u + mean_u * mean_v * count
    gvv = sum_vv - 2.0 * mean_v * sum_v + mean_v * mean_v * count
    ridge = 0.001 * count + 1.0
    diag_u = guu + ridge
    diag_v = gvv + ridge
    inverse = 1.0 / (diag_u * diag_v - guv * guv)
    base = 1.0 / (count + ridge)
    out = []
    slopes_u, slopes_v = [], []
    for h0, hu, hv in ((h0_re, hu_re, hv_re), (h0_im, hu_im, hv_im)):
        hu = hu - mean_u * h0
        hv = hv - mean_v * h0
        out.append(h0 * base)
        slopes_u.append((diag_v * hu - guv * hv) * inverse)
        slopes_v.append((diag_u * hv - guv * hu) * inverse)
    entries = out + slopes_u + slopes_v + [mean_u, mean_v]
    stacked = jnp.zeros((16, LANES), F32)
    place = row_of((16, LANES))
    for i, entry in enumerate(entries):
        stacked = jnp.where(place == i, entry, stacked)
    stacked = jnp.where(lane_of((16, LANES)) < SWEEP_TALLY, stacked, 0.0)
    high, middle, low = (across_lanes(membership[3], x) for x in split_three(stacked))
    coefs[...] = high + middle + low


def ramp_kernel(count_rows, count_cols, gamma, size, coefs, deramped, coherence, out, sem):
    _, rows, cols = gamma.shape
    my_row = lax.axis_index("rows")
    my_col = lax.axis_index("cols")
    lane = lane_of((8, LANES))
    across_first = ((my_col * cols + lane).astype(F32) + 0.5) * (2.0 / (cols * count_cols)) - 1.0
    chunk = 16
    copies = [pltpu.make_async_copy(size, coherence, sem.at[0])]
    copies[0].start()
    for low in range(0, rows, chunk):
        @pl.loop(low // 8, (low + chunk) // 8)
        def _(group):
            start = pl.multiple_of(group * 8, 8)
            here = pl.ds(start, 8)
            line = coefs[here, :]
            along = ((my_row * rows + start + row_of((8, LANES))).astype(F32) + 0.5) * (
                2.0 / (rows * count_rows)
            ) - 1.0
            wide = [jnp.broadcast_to(line[:, q:q + 1], (8, LANES)) for q in range(8)]
            along = along - wide[7]
            base_re = wide[0] + wide[4] * along
            base_im = wide[1] + wide[5] * along
            centred = across_first - wide[6]
            for j in range(cols // LANES):
                there = pl.ds(j * LANES, LANES)
                du = centred + j * (LANES * 2.0 / (cols * count_cols))
                model_re = base_re + wide[2] * du
                model_im = base_im + wide[3] * du
                real, imag = gamma[0, here, there], gamma[1, here, there]
                out[0, here, there] = real * model_re + imag * model_im
                out[1, here, there] = imag * model_re - real * model_im

        here = pl.ds(low, chunk)
        copy = pltpu.make_async_copy(out.at[:, here, :], deramped.at[:, here, :], sem.at[len(copies)])
        copy.start()
        copies.append(copy)
    for copy in copies:
        copy.wait()


def on_device(count_rows, count_cols, lead, trail, flags, sweep):
    rows, cols = flags.shape
    wide = 2 * LANES
    tiles, between = cols // wide, rows - 2 * HALO
    vmem = pl.BlockSpec(memory_space=pltpu.VMEM)
    hbm = pl.BlockSpec(memory_space=pl.ANY)
    dma = pltpu.SemaphoreType.DMA
    V = pltpu.VMEM
    gamma, size, coefs = pl.pallas_call(
        functools.partial(gamma_kernel, count_rows, count_cols),
        out_shape=(V((2, rows, cols), F32), V((rows, cols), F32), V((rows, 16), F32)),
        in_specs=[hbm, hbm, hbm, hbm],
        out_specs=(vmem, vmem, vmem),
        scratch_shapes=[
            V((2, rows, cols), F32), V((2, rows, cols), F32), V((rows, cols), jnp.int32), V((1, rows), jnp.int32),
            V((4, 2 * rows, cols), BF16),
            V((3, HALO, cols), F32), V((3, HALO, cols), F32), V((3, HALO, cols), F32), V((3, HALO, cols), F32),
            V((2, HALO, LANES), F32), V((2, HALO, LANES), F32),
            V((2, 2, HALO, LANES), F32),
            V((rows, 2 * LANES), F32), V((2 * HALO, 2 * LANES), F32), V((2 * rows, 2 * LANES), BF16), V((4 * HALO, 2 * LANES), BF16),
            V((rows, 2 * rows), BF16), V((2 * HALO, 4 * HALO), BF16),
            V((4, 4 * HALO, cols), BF16), V((wide, wide), BF16), V((wide, wide), BF16),
            V((tiles, 4, between, wide), BF16), V((tiles, 4, between, wide), BF16),
            V((tiles, 4, between, wide), BF16), V((tiles, 4, between, wide), F32),
            V((4, 2 * HALO, cols), F32),
            V((tiles, 4, 2 * HALO, wide), BF16), V((tiles, 4, 2 * HALO, wide), BF16),
            V((tiles, 4, 2 * HALO, wide), BF16), V((tiles, 4, 2 * HALO, wide), F32),
            V((7, between, LANES), F32), V((7, 2 * HALO, LANES), F32),
            V((rows, LANES), F32), V((4, LANES, rows), BF16),
            V((4, LANES), F32), V((PEERS, 4, LANES), F32), V((4, LANES), F32), V((REACH, 4, LANES), F32),
            dma((64,)), dma((2 * PARTS,)), dma((2 * PARTS,)), dma((4,)), dma((4,)), dma((PEERS,)), dma((PEERS,)),
            dma((REACH,)), dma((REACH,)), pltpu.SemaphoreType.REGULAR((5,)),
        ],
        compiler_params=pltpu.CompilerParams(
            collective_id=0, has_side_effects=True, vmem_limit_bytes=63_000_000
        ),
        name="coherence",
    )(lead, trail, flags, sweep.reshape(1, rows))
    return pl.pallas_call(
        functools.partial(ramp_kernel, count_rows, count_cols),
        out_shape=(
            jax.ShapeDtypeStruct((2, rows, cols), F32),
            jax.ShapeDtypeStruct((rows, cols), F32),
        ),
        in_specs=[vmem, vmem, vmem],
        out_specs=(hbm, hbm),
        scratch_shapes=[V((2, rows, cols), F32), dma((9,))],
        compiler_params=pltpu.CompilerParams(vmem_limit_bytes=16 * 1024 * 1024),
        name="ramp",
    )(gamma, size, coefs)


def solution(mesh):
    in_specs = (P(None, "rows", "cols"), P(None, "rows", "cols"), P("rows", "cols"), P("rows"))
    out_specs = (P(None, "rows", "cols"), P("rows", "cols"))
    body = functools.partial(on_device, mesh.shape["rows"], mesh.shape["cols"])
    return jax.shard_map(body, mesh=mesh, in_specs=in_specs, out_specs=out_specs, check_vma=False)
```
